16 devices in a mesh: sys: 4 (over z, y), row: 4 (over x, core).
Axes of the slice: x: 2, y: 2, z: 2, core: 2. Of those that a mesh axis runs over, the one named last changes fastest.
Arguments:
- positions: bfloat16 [32768, 128], P(('sys', 'row')), parts along dimension 0
- charges: float32 [32768], P(('sys', 'row')), parts along dimension 0
Outputs:
- output 1: float32 [32768, 128], P(('sys', 'row')), parts along dimension 0
- output 2: float32 [4], P('sys'), parts along dimension 0
There are 4 independent parts. The reference program is written for one: setup_inputs(seed, part) draws one part's arguments, and reference() takes and returns one part's arrays. A program takes and returns all parts, laid end to end along the dimension named above; each array names one.
All inputs are finite; a program needn't handle non-finite values.
Results may differ from the reference program's by a relative error of at most 0.001.
Values are sent between devices in bfloat16 or wider.
A program may use at most 1 GiB of HBM per device.

```python
import jax
import jax.numpy as jnp
from jax import lax

D = 128
ROWS_DEV = 2048
RING = 4
N_ROWS = ROWS_DEV * RING
ELL_SQ = float(D)


def setup_inputs(seed: int = 0, part: int = 0) -> dict:
    root_key = jax.random.key(seed)
    part_key = jax.random.fold_in(root_key, part)
    key_x, key_q = jax.random.split(part_key)
    positions = jax.random.normal(key_x, (N_ROWS, D), jnp.float32).astype(jnp.bfloat16)
    charges = jax.random.normal(key_q, (N_ROWS,), jnp.float32) * (N_ROWS ** -0.25)
    return {"positions": positions, "charges": charges}


def reference(positions, charges):
    sq_norm = jnp.sum(jnp.square(positions.astype(jnp.float32)), axis=1)
    blocks_x = positions.reshape(RING, ROWS_DEV, D)
    blocks_q = charges.reshape(RING, ROWS_DEV)
    blocks_sq = sq_norm.reshape(RING, ROWS_DEV)
    block_ids = jnp.arange(RING)
    local_ids = jnp.arange(ROWS_DEV)

    def row_block(host_in):
        host_x, host_q, host_sq, host_id = host_in

        def col_step(acc_state, col_in):
            force_acc, energy_acc = acc_state
            col_x, col_q, col_sq, col_id = col_in
            cross_dot = jnp.dot(host_x, col_x.T, preferred_element_type=jnp.float32)
            sq_dist = jnp.maximum(host_sq[:, None] + col_sq[None, :] - 2.0 * cross_dot, 0.0)
            is_self = (host_id * ROWS_DEV + local_ids)[:, None] == (col_id * ROWS_DEV + local_ids)[None, :]
            weight = jnp.where(is_self, 0.0, host_q[:, None] * col_q[None, :] * jnp.exp(-sq_dist / (2.0 * ELL_SQ)))
            pulled = jnp.dot(weight.astype(jnp.bfloat16), col_x, preferred_element_type=jnp.float32)
            force_acc = force_acc + jnp.sum(weight, axis=1)[:, None] * host_x.astype(jnp.float32) - pulled
            return (force_acc, energy_acc + jnp.sum(weight)), None

        init_state = (jnp.zeros((ROWS_DEV, D), jnp.float32), jnp.zeros((), jnp.float32))
        final_state, step_out = lax.scan(col_step, init_state, (blocks_x, blocks_q, blocks_sq, block_ids))
        return final_state

    forces, energies = lax.map(row_block, (blocks_x, blocks_q, blocks_sq, block_ids))
    return (forces / ELL_SQ).reshape(N_ROWS, D), (0.5 * jnp.sum(energies)).reshape(1)
```

```python
import functools
import math

import jax
import jax.numpy as jnp
from jax import lax
from jax.experimental import pallas as pl
from jax.experimental.pallas import tpu as pltpu
from jax.sharding import PartitionSpec as P

MESH = pl.DeviceIdType.MESH
T = 256
F32 = jnp.float32
BF16 = jnp.bfloat16
PIECE = 64


def split3(v):
    hi = v.astype(BF16).astype(F32)
    rest = v - hi
    mid = rest.astype(BF16).astype(F32)
    return hi, mid, rest - mid


def kernel(rows, feat, chunk, x_ref, q_ref, f_ref, e_ref, xall, qall, aug, xt, qb, rhs, qi, rs, ft, ebuf,
           xsend, xrecv, fsend, frecv, psend, precv, qsend, qrecv, esend, erecv):
    me = lax.axis_index("row")
    partner = me + 1 - 2 * lax.rem(me, 2)
    across = lax.rem(me + 2, 4)
    diagonal = lax.rem(partner + 2, 4)
    peers = (partner, across, diagonal)
    n_chunks = rows // chunk
    tiles = rows // T
    pairs = tiles // 2
    scale = math.log2(math.e) / (2.0 * feat)

    barrier = pltpu.get_barrier_semaphore()
    for peer in peers:
        pl.semaphore_signal(barrier, inc=1, device_id={"row": peer}, device_id_type=MESH)
    pl.semaphore_wait(barrier, 3)

    def remote(src, dst, ssem, rsem, peer):
        return pltpu.make_async_remote_copy(src_ref=src, dst_ref=dst, send_sem=ssem, recv_sem=rsem,
                                            device_id={"row": peer}, device_id_type=MESH)

    q_copies = [remote(q_ref, qall.at[k], qsend.at[k], qrecv.at[k], peer) for k, peer in enumerate(peers)]
    p_copy = remote(x_ref, xall.at[0], psend, precv, partner)
    def x_copy(c):
        part = pl.ds(pl.multiple_of(c * chunk, chunk), chunk)
        return remote(x_ref.at[part], xall.at[1, part], xsend.at[c], xrecv.at[c], across)

    def f_copy(c):
        part = pl.ds(pl.multiple_of(c * chunk, chunk), chunk)
        return remote(xall.at[1, part], xall.at[2, part], fsend.at[c], frecv.at[c], partner)
    for k in (1, 2):
        q_copies[k].start()
    for c in range(n_chunks):
        x_copy(c).start()
    q_copies[0].start()
    p_copy.start()

    row_id = lax.broadcasted_iota(jnp.int32, (8, T), 0)

    def prepare(x_val, q_row, row0, n):
        for k in range(n // T):
            part = x_val[k * T:(k + 1) * T]
            x_t = part.T
            xt[:, pl.ds(row0 + k * T, T)] = x_t
            wide = x_t.astype(F32)
            sq = jnp.sum(wide * wide, axis=0, keepdims=True)
            hi, mid, lo = split3(sq)
            block = jnp.where(row_id == 0, hi, jnp.where(row_id == 1, mid, jnp.where(row_id == 2, lo, jnp.where(row_id < 6, 1.0, 0.0))))
            block = jnp.concatenate([block, jnp.zeros((120, T), F32)], axis=0)
            aug[pl.ds(row0 + k * T, T), :] = block.T.astype(BF16)
            qb[pl.ds(row0 + k * T, T), :] = jnp.broadcast_to(q_row[:, k * T:(k + 1) * T], (128, T)).T
            yield k, x_t, (hi, mid, lo)

    def q_rows(ref):
        return ref[...].reshape(1, rows)

    q_own = q_rows(q_ref)
    qi[...] = jnp.broadcast_to(q_own, (8, rows))
    rs[...] = jnp.zeros_like(rs)
    ft[...] = jnp.zeros_like(ft)
    for k, x_t, (hi, mid, lo) in prepare(x_ref[...], q_own, 0, rows):
        cols = pl.ds(k * T, T)
        rhs[pl.ds(0, feat), cols] = x_t + x_t
        block = jnp.where(row_id < 3, -1.0, jnp.where(row_id == 3, -hi, jnp.where(row_id == 4, -mid, jnp.where(row_id == 5, -lo, 0.0))))
        rhs[pl.ds(feat, 128), cols] = jnp.concatenate([block, jnp.zeros((120, T), F32)], axis=0).astype(BF16)

    def main():
        def first(x_block, row0, t):
            lhs = jnp.concatenate([x_block, aug[pl.ds(row0, T), :]], axis=1)
            return jnp.dot(lhs, rhs[:, 2 * t * T:2 * (t + 1) * T], preferred_element_type=F32)

        def second(s, row0, t, mask_row):
            n = 2 * T
            cols = pl.ds(t * n, n)
            qi_t = qi[:, cols]
            total = rs[:, cols]
            out = []
            for p in range(T // PIECE):
                e = jnp.exp2(jnp.minimum(s[p * PIECE:(p + 1) * PIECE], 0.0) * scale)
                qj = qb[pl.ds(row0 + p * PIECE, PIECE), :]
                qq = (jnp.concatenate([qj] * 4, axis=1).reshape(PIECE // 8, 8, n) * qi_t[None]).reshape(PIECE, n)
                w = qq * e
                if mask_row is not None:
                    r = lax.broadcasted_iota(jnp.int32, (PIECE, n), 0) - lax.broadcasted_iota(jnp.int32, (PIECE, n), 1)
                    w = jnp.where(r == (t * n - p * PIECE) - mask_row, 0.0, w)
                total = total + jnp.sum(w.reshape(PIECE // 8, 8, n), axis=0)
                out.append(w.astype(BF16))
            rs[:, cols] = total
            ft[:, cols] += jnp.dot(xt[:, pl.ds(row0, T)], jnp.concatenate(out, axis=0), preferred_element_type=F32)

        def block_rows(x_of, row0, mask_row=None):
            x_block = x_of()
            ready = first(x_block, row0, 0)
            for t in range(pairs):
                following = first(x_block, row0, t + 1) if t + 1 < pairs else None
                second(ready, row0, t, mask_row)
                ready = following

        def own_step(c, carry):
            off = pl.multiple_of(c * T, T)
            block_rows(lambda: x_ref[pl.ds(off, T), :], off, off)
            return carry
        lax.fori_loop(0, tiles, own_step, 0)

        def other(slot, first_row, n):
            def step(k, carry):
                off = pl.multiple_of(first_row + k * T, T)
                base = pl.multiple_of((slot + 1) * rows + off, T)
                q_row = qall[slot, pl.ds(off // 128, T // 128), :].reshape(1, T)
                for _ in prepare(xall[slot, pl.ds(off, T), :], q_row, base, T):
                    pass
                block_rows(lambda: xall[slot, pl.ds(off, T), :], base)
                return carry
            lax.fori_loop(0, n // T, step, 0)

        q_copies[0].wait_recv()
        p_copy.wait_recv()
        other(0, 0, rows)
        for k in (1, 2):
            q_copies[k].wait_recv()
        def remote_chunk(c, carry):
            x_copy(c).wait_recv()
            f_copy(c).start()
            other(1, c * chunk, chunk)
            return carry
        lax.fori_loop(0, n_chunks, remote_chunk, 0)
        def forwarded_chunk(c, carry):
            f_copy(c).wait_recv()
            other(2, c * chunk, chunk)
            return carry
        lax.fori_loop(0, n_chunks, forwarded_chunk, 0)

        sums = jnp.sum(rs[...], axis=0, keepdims=True)
        energy = 0.5 * jnp.sum(sums, axis=1, keepdims=True)
        ebuf[me] = jnp.broadcast_to(energy, (8, 128))
        inv = 1.0 / feat
        def finish(t, m):
            tile = 2 * t + m
            cols = pl.ds(tile * T, T)
            pulled = ft[:, cols]
            force = (sums[:, tile * T:(tile + 1) * T] * xt[:, cols].astype(F32) - pulled) * inv
            f_ref[pl.ds(tile * T, T), :] = force.T
        finish(0, 0)
        finish(0, 1)
        e_copies = [remote(ebuf.at[me], ebuf.at[me], esend.at[k], erecv.at[k], peer) for k, peer in enumerate(peers)]
        for copy in e_copies:
            copy.start()
        for t in range(1, pairs):
            for m in range(2):
                finish(t, m)
        for copy in e_copies:
            copy.wait_recv()
        everything = (ebuf[0] + ebuf[1]) + (ebuf[2] + ebuf[3])
        e_ref[...] = everything
        for copy in e_copies + q_copies + [p_copy] + [x_copy(c) for c in range(n_chunks)] + [f_copy(c) for c in range(n_chunks)]:
            copy.wait_send()

    main()


def solution(mesh):
    def device_body(pos_loc, chg_loc):
        rows, feat = pos_loc.shape
        chunk = rows // 4
        n = 4
        DMA = pltpu.SemaphoreType.DMA
        call = pl.pallas_call(
            functools.partial(kernel, rows, feat, chunk),
            out_shape=[jax.ShapeDtypeStruct((rows, feat), F32), jax.ShapeDtypeStruct((8, 128), F32)],
            in_specs=[pl.BlockSpec(memory_space=pltpu.VMEM)] * 2,
            out_specs=[pl.BlockSpec(memory_space=pltpu.VMEM)] * 2,
            scratch_shapes=[
                pltpu.VMEM((3, rows, feat), BF16),
                pltpu.VMEM((3, rows // 128, 128), F32),
                pltpu.VMEM((n * rows, 128), BF16),
                pltpu.VMEM((feat, n * rows), BF16),
                pltpu.VMEM((n * rows, 128), F32),
                pltpu.VMEM((2 * 128, rows), BF16),
                pltpu.VMEM((8, rows), F32),
                pltpu.VMEM((8, rows), F32),
                pltpu.VMEM((feat, rows), F32),
                pltpu.VMEM((n, 8, 128), F32),
                DMA((4,)), DMA((4,)), DMA((4,)), DMA((4,)), DMA, DMA, DMA((3,)), DMA((3,)), DMA((3,)), DMA((3,)),
            ],
            compiler_params=pltpu.CompilerParams(collective_id=0, has_side_effects=True, vmem_limit_bytes=48 * 1024 * 1024),
        )
        force, energy = call(pos_loc, chg_loc.reshape(rows // 128, 128))
        return force, energy[0, :1]

    return jax.shard_map(device_body, mesh=mesh, in_specs=(P(("sys", "row"), None), P(("sys", "row"))), out_specs=(P(("sys", "row"), None), P("sys")), check_vma=False)
```

```python
import functools
import math

import jax
import jax.numpy as jnp
from jax import lax
from jax.experimental import pallas as pl
from jax.experimental.pallas import tpu as pltpu
from jax.sharding import PartitionSpec as P

MESH = pl.DeviceIdType.MESH
T = 256
F32 = jnp.float32
BF16 = jnp.bfloat16
PIECE = 64


def split3(v):
    hi = v.astype(BF16).astype(F32)
    rest = v - hi
    mid = rest.astype(BF16).astype(F32)
    return hi, mid, rest - mid


def kernel(rows, feat, x_ref, q_ref, f_ref, e_ref, xall, qall, aug, xt, qb, rhs, qi, rs, ft, ebuf,
           xsend, xrecv, fsend, frecv, psend, precv, qsend, qrecv, esend, erecv):
    me = lax.axis_index("row")
    partner = me + 1 - 2 * lax.rem(me, 2)
    across = lax.rem(me + 2, 4)
    diagonal = lax.rem(partner + 2, 4)
    peers = (partner, across, diagonal)
    chunk = 2 * T
    n_chunks = rows // chunk
    lanes = chunk // 128
    scale = math.log2(math.e) / (2.0 * feat)

    barrier = pltpu.get_barrier_semaphore()
    for peer in peers:
        pl.semaphore_signal(barrier, inc=1, device_id={"row": peer}, device_id_type=MESH)
    pl.semaphore_wait(barrier, 3)

    def remote(src, dst, ssem, rsem, peer):
        return pltpu.make_async_remote_copy(src_ref=src, dst_ref=dst, send_sem=ssem, recv_sem=rsem,
                                            device_id={"row": peer}, device_id_type=MESH)

    def part(c):
        return pl.ds(pl.multiple_of(c * chunk, chunk), chunk)

    q_copies = [remote(q_ref, qall.at[k], qsend.at[k], qrecv.at[k], peer) for k, peer in enumerate(peers)]

    def p_copy(c):
        return remote(x_ref.at[part(c)], xall.at[0, part(c)], psend.at[c], precv.at[c], partner)

    def x_copy(c):
        return remote(x_ref.at[part(c)], xall.at[1, part(c)], xsend.at[c], xrecv.at[c], across)

    def f_copy(c):
        return remote(xall.at[1, part(c)], xall.at[2, part(c)], fsend.at[c], frecv.at[c], partner)

    for k in (1, 2, 0):
        q_copies[k].start()
    for c in range(n_chunks):
        x_copy(c).start()
        p_copy(c).start()

    row_id = lax.broadcasted_iota(jnp.int32, (8, chunk), 0)
    filler = jnp.zeros((120, chunk), BF16)

    def prepare(x_val, q_row, g):
        x_t = x_val.T
        for k in range(lanes):
            xt[g * lanes + k] = x_t[:, k * 128:(k + 1) * 128]
        wide = x_t.astype(F32)
        hi, mid, lo = split3(jnp.sum(wide * wide, axis=0, keepdims=True))
        block = jnp.where(row_id == 0, hi, jnp.where(row_id == 1, mid, jnp.where(row_id == 2, lo, jnp.where(row_id < 6, 1.0, 0.0))))
        aug[g] = jnp.concatenate([block, jnp.zeros((120, chunk), F32)], axis=0).astype(BF16).T
        qb[g] = jnp.broadcast_to(q_row, (128, chunk)).T
        return x_t, hi, mid, lo

    def q_rows(ref, c):
        return ref[pl.ds(c * lanes, lanes), :].reshape(1, chunk)

    rs[...] = jnp.zeros_like(rs)
    ft[...] = jnp.zeros_like(ft)
    for c in range(n_chunks):
        q_row = q_rows(q_ref, c)
        qi[c] = jnp.broadcast_to(q_row, (8, chunk))
        x_t, hi, mid, lo = prepare(x_ref[pl.ds(c * chunk, chunk), :], q_row, c)
        block = jnp.where(row_id < 3, -1.0, jnp.where(row_id == 3, -hi, jnp.where(row_id == 4, -mid, jnp.where(row_id == 5, -lo, 0.0))))
        block = jnp.concatenate([block, jnp.zeros((120, chunk), F32)], axis=0).astype(BF16)
        double = x_t + x_t
        for k in range(lanes):
            rhs[c, k, pl.ds(0, feat), :] = double[:, k * 128:(k + 1) * 128]
            rhs[c, k, pl.ds(feat, 128), :] = block[:, k * 128:(k + 1) * 128]

    def wide_load(ref, i):
        return jnp.concatenate([ref[i, k] for k in range(lanes)], axis=1)

    def first(x_of, g, h, t):
        lhs = jnp.concatenate([x_of(h), aug[g, pl.ds(h * T, T), :]], axis=1)
        return jnp.dot(lhs, wide_load(rhs, t), preferred_element_type=F32)

    def weights(s, g, h, t, masked):
        qi_t = qi[t]
        total = rs[t]
        out = []
        for p in range(T // PIECE):
            e = jnp.exp2(jnp.minimum(s[p * PIECE:(p + 1) * PIECE], 0.0) * scale)
            qj = qb[g, pl.ds(h * T + p * PIECE, PIECE), :]
            qq = (jnp.concatenate([qj] * lanes, axis=1).reshape(PIECE // 8, 8, chunk) * qi_t[None]).reshape(PIECE, chunk)
            w = qq * e
            if masked:
                r = lax.broadcasted_iota(jnp.int32, (PIECE, chunk), 0) + (h * T + p * PIECE)
                w = jnp.where(r == lax.broadcasted_iota(jnp.int32, (PIECE, chunk), 1), 0.0, w)
            total = total + jnp.sum(w.reshape(PIECE // 8, 8, chunk), axis=0)
            out.append(w.astype(BF16))
        rs[t] = total
        return jnp.concatenate(out, axis=0)

    def chunk_rows(x_of, g, groups):
        steps = [(t, h, m) for t, m in groups for h in range(2)]
        ready = first(x_of, g, steps[0][1], steps[0][0])
        got = []
        for n, (t, h, m) in enumerate(steps):
            following = first(x_of, g, steps[n + 1][1], steps[n + 1][0]) if n + 1 < len(steps) else None
            got.append(weights(ready, g, h, t, m))
            if h == 1:
                lhs = jnp.concatenate([xt[g * lanes + k] for k in range(lanes)], axis=1)
                ft[t] += jnp.dot(lhs, jnp.concatenate(got, axis=0), preferred_element_type=F32)
                got = []
            ready = following

    def arrive(slot, c):
        if slot == 0:
            p_copy(c).wait_recv()
        elif slot == 1:
            x_copy(c).wait_recv()
            f_copy(c).start()
        else:
            f_copy(c).wait_recv()

    for slot in range(n_chunks):
        for k in ((0,), (1, 2), (), ())[slot]:
            q_copies[k].wait_recv()

        def body(c, carry, slot=slot):
            if slot < 3:
                arrive(slot, c)
                prepare(xall[slot, part(c), :], q_rows(qall.at[slot], c), (slot + 1) * n_chunks + c)
            if slot == 0:
                x_of = lambda h: x_ref[pl.ds(pl.multiple_of(c * chunk + h * T, T), T), :]
                groups = [(lax.rem(c + k, n_chunks), k == 0) for k in range(n_chunks)]
            else:
                x_of = lambda h: xall[slot - 1, pl.ds(pl.multiple_of(c * chunk + h * T, T), T), :]
                groups = [(k, False) for k in range(n_chunks)]
            chunk_rows(x_of, slot * n_chunks + c, groups)
            return carry
        lax.fori_loop(0, n_chunks, body, 0)

    sums = [jnp.sum(rs[t], axis=0, keepdims=True) for t in range(n_chunks)]
    energy = 0.5 * jnp.sum((sums[0] + sums[1]) + (sums[2] + sums[3]), axis=1, keepdims=True)
    ebuf[me] = jnp.broadcast_to(energy, (8, 128))
    inv = 1.0 / feat

    def finish(t):
        own = jnp.concatenate([xt[t * lanes + k] for k in range(lanes)], axis=1).astype(F32)
        f_ref[pl.ds(t * chunk, chunk), :] = ((sums[t] * own - ft[t]) * inv).T

    finish(0)
    e_copies = [remote(ebuf.at[me], ebuf.at[me], esend.at[k], erecv.at[k], peer) for k, peer in enumerate(peers)]
    for copy in e_copies:
        copy.start()
    for t in range(1, n_chunks):
        finish(t)
    for copy in e_copies:
        copy.wait_recv()
    e_ref[...] = (ebuf[0] + ebuf[1]) + (ebuf[2] + ebuf[3])
    for copy in e_copies + q_copies + [f(c) for f in (p_copy, x_copy, f_copy) for c in range(n_chunks)]:
        copy.wait_send()


def solution(mesh):
    def device_body(pos_loc, chg_loc):
        rows, feat = pos_loc.shape
        chunk, n = 2 * T, 4
        own = rows // chunk
        DMA = pltpu.SemaphoreType.DMA
        call = pl.pallas_call(
            functools.partial(kernel, rows, feat),
            out_shape=[jax.ShapeDtypeStruct((rows, feat), F32), jax.ShapeDtypeStruct((8, 128), F32)],
            in_specs=[pl.BlockSpec(memory_space=pltpu.VMEM)] * 2,
            out_specs=[pl.BlockSpec(memory_space=pltpu.VMEM)] * 2,
            scratch_shapes=[
                pltpu.VMEM((3, rows, feat), BF16),
                pltpu.VMEM((3, rows // 128, 128), F32),
                pltpu.VMEM((n * own, chunk, 128), BF16),
                pltpu.VMEM((n * rows // 128, feat, 128), BF16),
                pltpu.VMEM((n * own, chunk, 128), F32),
                pltpu.VMEM((own, chunk // 128, 2 * 128, 128), BF16),
                pltpu.VMEM((own, 8, chunk), F32),
                pltpu.VMEM((own, 8, chunk), F32),
                pltpu.VMEM((own, feat, chunk), F32),
                pltpu.VMEM((n, 8, 128), F32),
                DMA((own,)), DMA((own,)), DMA((own,)), DMA((own,)), DMA((own,)), DMA((own,)), DMA((3,)), DMA((3,)), DMA((3,)), DMA((3,)),
            ],
            compiler_params=pltpu.CompilerParams(collective_id=0, has_side_effects=True, vmem_limit_bytes=48 * 1024 * 1024),
        )
        force, energy = call(pos_loc, chg_loc.reshape(rows // 128, 128))
        return force, energy[0, :1]

    return jax.shard_map(device_body, mesh=mesh, in_specs=(P(("sys", "row"), None), P(("sys", "row"))), out_specs=(P(("sys", "row"), None), P("sys")), check_vma=False)
```

```python
import functools
import math

import jax
import jax.numpy as jnp
from jax import lax
from jax.experimental import pallas as pl
from jax.experimental.pallas import tpu as pltpu
from jax.sharding import PartitionSpec as P

MESH = pl.DeviceIdType.MESH
T = 256
F32 = jnp.float32
BF16 = jnp.bfloat16
PIECE = 64


def split3(v):
    hi = v.astype(BF16).astype(F32)
    rest = v - hi
    mid = rest.astype(BF16).astype(F32)
    return hi, mid, rest - mid


def kernel(rows, feat, x_ref, q_ref, f_ref, e_ref, xall, qall, aug, xt, qb, rhs, qi, rs, ft, sbuf, wbuf, ebuf,
           lsem, xsend, xrecv, fsend, frecv, psend, precv, qsend, qrecv, esend, erecv):
    me = lax.axis_index("row")
    upper = me // 2
    partner = me + 1 - 2 * lax.rem(me, 2)
    third = (1 - upper) * (3 - me) + upper * (me - 2)
    last = third + 1 - 2 * lax.rem(third, 2)
    peers = (partner, third, last)
    chunk = 2 * T
    own = rows // chunk
    total = 4 * own
    half = own // 2
    lanes = chunk // 128
    scale = math.log2(math.e) / (2.0 * feat)

    local = [pltpu.make_async_copy(q_ref, qall.at[pl.ds(0, own * lanes)], lsem.at[own])]
    local += [pltpu.make_async_copy(x_ref.at[c], xall.at[c], lsem.at[c]) for c in range(own)]
    for copy in local:
        copy.start()
    barrier = pltpu.get_barrier_semaphore()
    for peer in peers:
        pl.semaphore_signal(barrier, inc=1, device_id={"row": peer}, device_id_type=MESH)

    def remote(src, dst, ssem, rsem, peer):
        return pltpu.make_async_remote_copy(src_ref=src, dst_ref=dst, send_sem=ssem, recv_sem=rsem,
                                            device_id={"row": peer}, device_id_type=MESH)

    q_copies = [remote(q_ref, qall.at[pl.ds((k + 1) * own * lanes, own * lanes)], qsend.at[k], qrecv.at[k], peer)
                for k, peer in enumerate(peers)]
    p_copy = remote(xall.at[pl.ds(0, own)], xall.at[pl.ds(own, own)], psend, precv, partner)
    x_copies = [remote(xall.at[pl.ds(k * half, half)], xall.at[pl.ds(2 * own + k * half, half)], xsend.at[k], xrecv.at[k], third)
                for k in range(2)]
    f_copies = [remote(xall.at[pl.ds(2 * own + k * half, half)], xall.at[pl.ds(3 * own + k * half, half)], fsend.at[k], frecv.at[k], partner)
                for k in range(2)]

    row_id = lax.broadcasted_iota(jnp.int32, (8, chunk), 0)
    filler = jnp.zeros((120, chunk), F32)

    def norms(x_t):
        wide = x_t.astype(F32)
        return split3(jnp.sum(wide * wide, axis=0, keepdims=True))

    def q_row(g):
        return qall[pl.ds(g * lanes, lanes), :].reshape(1, chunk)

    def prepare(g, side):
        x_t = xall[g].T
        hi, mid, lo = norms(x_t)
        block = jnp.where(row_id == 0, hi, jnp.where(row_id == 1, mid, jnp.where(row_id == 2, lo, jnp.where(row_id < 6, 1.0, 0.0))))
        aug[side] = jnp.concatenate([block, filler], axis=0).astype(BF16).T
        qb[side] = jnp.broadcast_to(q_row(g), (128, chunk)).T
        for k in range(lanes):
            xt[side, k] = x_t[:, k * 128:(k + 1) * 128]

    def wide_load(ref, i):
        return jnp.concatenate([ref[i, k] for k in range(lanes)], axis=1)

    def first(g, side, h, t):
        lhs = jnp.concatenate([xall[g, pl.ds(h * T, T), :], aug[side, pl.ds(h * T, T), :]], axis=1)
        return jnp.dot(lhs, wide_load(rhs, t), preferred_element_type=F32)

    def weights(s, side, h, t, phase, masked, keep):
        qi_t = qi[t]
        acc = rs[phase, t]
        for p in range(T // PIECE):
            e = jnp.exp2(jnp.minimum(s(p), 0.0) * scale)
            rows_p = pl.ds(h * T + p * PIECE, PIECE)
            qj = qb[side, rows_p, :]
            qq = (jnp.concatenate([qj] * lanes, axis=1).reshape(PIECE // 8, 8, chunk) * qi_t[None]).reshape(PIECE, chunk)
            w = qq * e
            if masked:
                r = lax.broadcasted_iota(jnp.int32, (PIECE, chunk), 0) + (h * T + p * PIECE)
                w = jnp.where(r == lax.broadcasted_iota(jnp.int32, (PIECE, chunk), 1), 0.0, w)
            acc = acc + jnp.sum(w.reshape(PIECE // 8, 8, chunk), axis=0)
            w = w.astype(BF16)
            for j in range(lanes):
                wbuf[keep, j, rows_p, :] = w[:, j * 128:(j + 1) * 128]
        rs[phase, t] = acc

    def pull(side, t, keep):
        ft[t] += jnp.dot(wide_load(xt, side), wide_load(wbuf, keep), preferred_element_type=F32)

    def body(g, side, order, before, phase, masked=False, prep=True):
        steps = [(k, h) for k in range(own) for h in range(2)]
        ready = lambda p: sbuf[pl.ds(p * PIECE, PIECE), :]
        for n, (k, h) in enumerate(steps):
            if n + 1 < len(steps):
                following = first(g, side, steps[n + 1][1], order[steps[n + 1][0]])
            if h == 0:
                if k == 0:
                    pull(1 - side, before, 1)
                else:
                    pull(side, order[k - 1], (k - 1) % 2)
            if n == 0 and prep:
                prepare(g + 1, 1 - side)
            weights(ready, side, h, order[k], phase, masked and k == 0, k % 2)
            ready = lambda p, v=following: v[p * PIECE:(p + 1) * PIECE]
        if prep:
            sbuf[...] = first(g + 1, 1 - side, 0, prep[0] if isinstance(prep, list) else 0)

    rs[...] = jnp.zeros_like(rs)
    ft[...] = jnp.zeros_like(ft)
    wbuf[1] = jnp.zeros_like(wbuf[1])
    xt[1] = jnp.zeros_like(xt[1])
    local[0].wait()
    for c in range(own):
        local[1 + c].wait()
        qi[c] = jnp.broadcast_to(q_row(c), (8, chunk))
        x_t = xall[c].T
        hi, mid, lo = norms(x_t)
        block = jnp.where(row_id < 3, -1.0, jnp.where(row_id == 3, -hi, jnp.where(row_id == 4, -mid, jnp.where(row_id == 5, -lo, 0.0))))
        block = jnp.concatenate([block, filler], axis=0).astype(BF16)
        double = x_t + x_t
        for k in range(lanes):
            rhs[c, k, pl.ds(0, feat), :] = double[:, k * 128:(k + 1) * 128]
            rhs[c, k, pl.ds(feat, 128), :] = block[:, k * 128:(k + 1) * 128]
    prepare(0, 0)
    sbuf[...] = first(0, 0, 0, 0)

    pl.semaphore_wait(barrier, 3)
    for k in (1, 2, 0):
        q_copies[k].start()
    for copy in x_copies + [p_copy]:
        copy.start()

    fixed = list(range(own))
    for g in range(own):
        if g == own - 1:
            q_copies[0].wait_recv()
            p_copy.wait_recv()
        body(g, g % 2, fixed[g:] + fixed[:g], (g + own - 2) % own, 0, masked=True, prep=[(g + 1) % own])

    def two(i, carry, phase, before):
        g = own + 2 * i
        body(g, 0, fixed, own - 1, phase)
        @pl.when(g + 1 == 2 * own - 1)
        def _():
            q_copies[1].wait_recv()
            q_copies[2].wait_recv()
            x_copies[0].wait_recv()
            f_copies[0].start()

        @pl.when(g + 1 == 2 * own + half - 1)
        def _():
            x_copies[1].wait_recv()
            f_copies[1].start()
        @pl.when(g + 1 == 3 * own - 1)
        def _():
            f_copies[0].wait_recv()
        body(g + 1, 1, fixed, own - 1, phase)
        return carry
    body(own, 0, fixed, own - 2, 0)
    body(own + 1, 1, fixed, own - 1, 0)
    lax.fori_loop(1, own, lambda i, c: two(i, c, i // half, None), 0)

    def total_of(phase):
        sums = (rs[phase, 0] + rs[phase, 1]) + (rs[phase, 2] + rs[phase, 3])
        return jnp.sum(jnp.sum(sums, axis=0, keepdims=True), axis=1, keepdims=True)
    ebuf[me] = jnp.broadcast_to(0.5 * total_of(0) + total_of(1), (8, 128))
    e_copies = [remote(ebuf.at[me], ebuf.at[me], esend.at[k], erecv.at[k], peer) for k, peer in enumerate(peers)]

    for g in range(3 * own, total):
        if g == 3 * own + half - 1:
            f_copies[1].wait_recv()
        if g == 3 * own + half:
            for copy in e_copies:
                copy.start()
        body(g, g % 2, fixed, own - 1, 2, prep=g + 1 < total)
    pull(1, own - 1, 1)

    inv = 1.0 / feat
    for t in range(own):
        sums = jnp.sum(rs[0, t] + rs[1, t] + rs[2, t], axis=0, keepdims=True)
        mine = xall[t].T.astype(F32)
        f_ref[pl.ds(t * chunk, chunk), :] = ((sums * mine - ft[t]) * inv).T
    for copy in e_copies:
        copy.wait_recv()
    e_ref[...] = (ebuf[0] + ebuf[1]) + (ebuf[2] + ebuf[3])
    for copy in e_copies + q_copies + [p_copy] + x_copies + f_copies:
        copy.wait_send()


def solution(mesh):
    def device_body(pos_loc, chg_loc):
        rows, feat = pos_loc.shape
        chunk = 2 * T
        own = rows // chunk
        total = 4 * own
        DMA = pltpu.SemaphoreType.DMA
        call = pl.pallas_call(
            functools.partial(kernel, rows, feat),
            out_shape=[jax.ShapeDtypeStruct((rows, feat), F32), jax.ShapeDtypeStruct((8, 128), F32)],
            in_specs=[pl.BlockSpec(memory_space=pl.ANY)] * 2,
            out_specs=[pl.BlockSpec(memory_space=pltpu.VMEM)] * 2,
            scratch_shapes=[
                pltpu.VMEM((total, chunk, feat), BF16),
                pltpu.VMEM((4 * rows // 128, 128), F32),
                pltpu.VMEM((2, chunk, 128), BF16),
                pltpu.VMEM((2, chunk // 128, feat, 128), BF16),
                pltpu.VMEM((2, chunk, 128), F32),
                pltpu.VMEM((own, chunk // 128, 2 * 128, 128), BF16),
                pltpu.VMEM((own, 8, chunk), F32),
                pltpu.VMEM((3, own, 8, chunk), F32),
                pltpu.VMEM((own, feat, chunk), F32),
                pltpu.VMEM((T, chunk), F32),
                pltpu.VMEM((2, chunk // 128, chunk, 128), BF16),
                pltpu.VMEM((4, 8, 128), F32),
                DMA((own + 1,)), DMA((2,)), DMA((2,)), DMA((2,)), DMA((2,)), DMA, DMA, DMA((3,)), DMA((3,)), DMA((3,)), DMA((3,)),
            ],
            compiler_params=pltpu.CompilerParams(collective_id=0, has_side_effects=True, vmem_limit_bytes=48 * 1024 * 1024),
        )
        force, energy = call(pltpu.with_memory_space_constraint(pos_loc.reshape(own, chunk, feat), pltpu.HBM),
                             pltpu.with_memory_space_constraint(chg_loc.reshape(rows // 128, 128), pltpu.HBM))
        return force, energy[0, :1]

    return jax.shard_map(device_body, mesh=mesh, in_specs=(P(("sys", "row"), None), P(("sys", "row"))), out_specs=(P(("sys", "row"), None), P("sys")), check_vma=False)
```

```python
import functools
import math

import jax
import jax.numpy as jnp
from jax import lax
from jax.experimental import pallas as pl
from jax.experimental.pallas import tpu as pltpu
from jax.sharding import PartitionSpec as P

MESH = pl.DeviceIdType.MESH
T = 256
F32 = jnp.float32
BF16 = jnp.bfloat16
PIECE = 64


def split3(v):
    hi = v.astype(BF16).astype(F32)
    rest = v - hi
    mid = rest.astype(BF16).astype(F32)
    return hi, mid, rest - mid


def kernel(rows, feat, x_ref, q_ref, ft, rs, ebuf, xall, qall, aug, xt, qb, rhs, top, sign, sbuf, wbuf,
           lsem, xsend, xrecv, fsend, frecv, psend, precv, qsend, qrecv, esend, erecv):
    me = lax.axis_index("row")
    upper = me // 2
    partner = me + 1 - 2 * lax.rem(me, 2)
    third = (1 - upper) * (3 - me) + upper * (me - 2)
    last = third + 1 - 2 * lax.rem(third, 2)
    peers = (partner, third, last)
    chunk = 2 * T
    own = rows // chunk
    total = 4 * own
    half = own // 2
    lanes = chunk // 128
    scale = math.log2(math.e) / (2.0 * feat)

    local = [pltpu.make_async_copy(q_ref, qall.at[pl.ds(0, own * lanes)], lsem.at[own])]
    local += [pltpu.make_async_copy(x_ref.at[c], xall.at[c], lsem.at[c]) for c in range(own)]
    for copy in local:
        copy.start()
    barrier = pltpu.get_barrier_semaphore()
    for peer in peers:
        pl.semaphore_signal(barrier, inc=1, device_id={"row": peer}, device_id_type=MESH)

    def remote(src, dst, ssem, rsem, peer):
        return pltpu.make_async_remote_copy(src_ref=src, dst_ref=dst, send_sem=ssem, recv_sem=rsem,
                                            device_id={"row": peer}, device_id_type=MESH)

    q_copies = [remote(q_ref, qall.at[pl.ds((k + 1) * own * lanes, own * lanes)], qsend.at[k], qrecv.at[k], peer)
                for k, peer in enumerate(peers)]
    p_copy = remote(xall.at[pl.ds(0, own)], xall.at[pl.ds(own, own)], psend, precv, partner)
    x_copies = [remote(xall.at[pl.ds(k * half, half)], xall.at[pl.ds(2 * own + k * half, half)], xsend.at[k], xrecv.at[k], third)
                for k in range(2)]
    f_copies = [remote(xall.at[pl.ds(2 * own + k * half, half)], xall.at[pl.ds(3 * own + k * half, half)], fsend.at[k], frecv.at[k], partner)
                for k in range(2)]

    row_id = lax.broadcasted_iota(jnp.int32, (8, chunk), 0)
    filler = jnp.zeros((120, chunk), F32)

    def norms(x_t):
        wide = x_t.astype(F32)
        return split3(jnp.sum(wide * wide, axis=0, keepdims=True))

    def q_row(g):
        return qall[pl.ds(g * lanes, lanes), :].reshape(1, chunk)

    def prepare(g, side):
        x_t = xall[g].T
        hi, mid, lo = norms(x_t)
        block = jnp.where(row_id == 0, hi, jnp.where(row_id == 1, mid, jnp.where(row_id == 2, lo, jnp.where(row_id < 6, 1.0, 0.0))))
        aug[side] = jnp.concatenate([block, filler], axis=0).astype(BF16).T
        qb[side] = jnp.broadcast_to(q_row(g), (128, chunk)).T
        for k in range(lanes):
            xt[side, k] = x_t[:, k * 128:(k + 1) * 128]

    def wide_load(ref, i):
        return jnp.concatenate([ref[i, k] for k in range(lanes)], axis=1)

    def first(g, side, h, t):
        lhs = jnp.concatenate([xall[g, pl.ds(h * T, T), :], aug[side, pl.ds(h * T, T), :]], axis=1)
        return jnp.dot(lhs, wide_load(rhs, t), preferred_element_type=F32)

    def weights(s, side, h, t, phase, masked, keep):
        top_t = top[t]
        acc = rs[phase, t]
        for p in range(T // PIECE):
            e = jnp.exp2(jnp.minimum(s(p).reshape(PIECE // 8, 8, chunk), top_t[None]) * scale).reshape(PIECE, chunk)
            rows_p = pl.ds(h * T + p * PIECE, PIECE)
            w = jnp.concatenate([qb[side, rows_p, :]] * lanes, axis=1) * e
            if masked:
                r = lax.broadcasted_iota(jnp.int32, (PIECE, chunk), 0) + (h * T + p * PIECE)
                w = jnp.where(r == lax.broadcasted_iota(jnp.int32, (PIECE, chunk), 1), 0.0, w)
            acc = acc + jnp.sum(w.reshape(PIECE // 8, 8, chunk), axis=0)
            w = w.astype(BF16)
            for j in range(lanes):
                wbuf[keep, j, rows_p, :] = w[:, j * 128:(j + 1) * 128]
        rs[phase, t] = acc

    def pull(side, t, keep):
        ft[t] += jnp.dot(wide_load(xt, side), wide_load(wbuf, keep), preferred_element_type=F32)

    def body(g, side, order, before, phase, masked=False, prep=True):
        steps = [(k, h) for k in range(own) for h in range(2)]
        ready = lambda p: sbuf[pl.ds(p * PIECE, PIECE), :]
        for n, (k, h) in enumerate(steps):
            if n + 1 < len(steps):
                following = first(g, side, steps[n + 1][1], order[steps[n + 1][0]])
            if h == 0:
                if k == 0:
                    pull(1 - side, before, 1)
                else:
                    pull(side, order[k - 1], (k - 1) % 2)
            if n == 0 and prep:
                prepare(g + 1, 1 - side)
            weights(ready, side, h, order[k], phase, masked and k == 0, k % 2)
            ready = lambda p, v=following: v[p * PIECE:(p + 1) * PIECE]
        if prep:
            sbuf[...] = first(g + 1, 1 - side, 0, prep[0] if isinstance(prep, list) else 0)

    rs[...] = jnp.zeros_like(rs)
    ft[...] = jnp.zeros_like(ft)
    wbuf[1] = jnp.zeros_like(wbuf[1])
    xt[1] = jnp.zeros_like(xt[1])
    local[0].wait()
    for c in range(own):
        local[1 + c].wait()
        q_c = q_row(c)
        sign[c] = jnp.broadcast_to(jnp.where(q_c < 0.0, -1.0, 1.0), (8, chunk))
        level = jnp.maximum(jnp.log2(jnp.abs(q_c)), -1000.0) * (1.0 / scale)
        top[c] = jnp.broadcast_to(level, (8, chunk))
        x_t = xall[c].T
        terms = [-1.0, -1.0, -1.0] + [v for v in split3(level - jnp.sum(jnp.square(x_t.astype(F32)), axis=0, keepdims=True))]
        block = jnp.zeros((8, chunk), F32)
        for k, v in enumerate(terms):
            block = jnp.where(row_id == k, v, block)
        block = jnp.concatenate([block, filler], axis=0).astype(BF16)
        double = x_t + x_t
        for k in range(lanes):
            rhs[c, k, pl.ds(0, feat), :] = double[:, k * 128:(k + 1) * 128]
            rhs[c, k, pl.ds(feat, 128), :] = block[:, k * 128:(k + 1) * 128]
    prepare(0, 0)
    sbuf[...] = first(0, 0, 0, 0)

    pl.semaphore_wait(barrier, 3)
    for k in (1, 2, 0):
        q_copies[k].start()
    for copy in x_copies + [p_copy]:
        copy.start()

    fixed = list(range(own))
    for g in range(own):
        if g == own - 1:
            q_copies[0].wait_recv()
            p_copy.wait_recv()
        body(g, g % 2, fixed[g:] + fixed[:g], (g + own - 2) % own, 0, masked=True, prep=[(g + 1) % own])

    def two(i, carry, phase, before):
        g = own + 2 * i
        body(g, 0, fixed, own - 1, phase)
        @pl.when(g + 1 == 2 * own - 1)
        def _():
            q_copies[1].wait_recv()
            q_copies[2].wait_recv()
            x_copies[0].wait_recv()
            f_copies[0].start()

        @pl.when(g + 1 == 2 * own + half - 1)
        def _():
            x_copies[1].wait_recv()
            f_copies[1].start()
        @pl.when(g + 1 == 3 * own - 1)
        def _():
            f_copies[0].wait_recv()
        body(g + 1, 1, fixed, own - 1, phase)
        return carry
    body(own, 0, fixed, own - 2, 0)
    body(own + 1, 1, fixed, own - 1, 0)
    lax.fori_loop(1, own, lambda i, c: two(i, c, i // half, None), 0)

    def total_of(phase):
        sums = (rs[phase, 0] * sign[0] + rs[phase, 1] * sign[1]) + (rs[phase, 2] * sign[2] + rs[phase, 3] * sign[3])
        return jnp.sum(jnp.sum(sums, axis=0, keepdims=True), axis=1, keepdims=True)
    ebuf[me] = jnp.broadcast_to(0.5 * total_of(0) + total_of(1), (8, 128))
    e_copies = [remote(ebuf.at[me], ebuf.at[me], esend.at[k], erecv.at[k], peer) for k, peer in enumerate(peers)]

    for g in range(3 * own, total):
        if g == 3 * own + half - 1:
            f_copies[1].wait_recv()
        if g == 3 * own + half:
            for copy in e_copies:
                copy.start()
        body(g, g % 2, fixed, own - 1, 2, prep=g + 1 < total)
    pull(1, own - 1, 1)

    for t in range(own):
        rs[0, t] = (rs[0, t] + rs[1, t]) + rs[2, t]
        rs[1, t] = sign[t]
    for copy in e_copies:
        copy.wait_recv()
    for copy in e_copies + q_copies + [p_copy] + x_copies + f_copies:
        copy.wait_send()


def finish(x_ref, ft, rs, ebuf, f_ref, e_ref, stage, sems):
    own, feat, chunk = ft.shape
    inv = 1.0 / feat
    copies = []
    for t in range(own):
        factor = rs[1, t, pl.ds(0, 1), :] * inv
        sums = jnp.sum(rs[0, t], axis=0, keepdims=True)
        stage[t] = ((sums * x_ref[t].T.astype(F32) - ft[t]) * factor).T
        copies.append(pltpu.make_async_copy(stage.at[t], f_ref.at[t], sems.at[t]))
        copies[-1].start()
    energy = (ebuf[0] + ebuf[1]) + (ebuf[2] + ebuf[3])
    e_ref[0] = jnp.max(energy[0:1, 0:1])
    for copy in copies:
        copy.wait()


def solution(mesh):
    def device_body(pos_loc, chg_loc):
        rows, feat = pos_loc.shape
        chunk = 2 * T
        own = rows // chunk
        total = 4 * own
        DMA = pltpu.SemaphoreType.DMA
        call = pl.pallas_call(
            functools.partial(kernel, rows, feat),
            out_shape=[jax.ShapeDtypeStruct((own, feat, chunk), F32), jax.ShapeDtypeStruct((3, own, 8, chunk), F32),
                       jax.ShapeDtypeStruct((4, 8, 128), F32)],
            in_specs=[pl.BlockSpec(memory_space=pl.ANY)] * 2,
            out_specs=[pl.BlockSpec(memory_space=pltpu.VMEM)] * 3,
            scratch_shapes=[
                pltpu.VMEM((total, chunk, feat), BF16),
                pltpu.VMEM((4 * rows // 128, 128), F32),
                pltpu.VMEM((2, chunk, 128), BF16),
                pltpu.VMEM((2, chunk // 128, feat, 128), BF16),
                pltpu.VMEM((2, chunk, 128), F32),
                pltpu.VMEM((own, chunk // 128, 2 * 128, 128), BF16),
                pltpu.VMEM((own, 8, chunk), F32),
                pltpu.VMEM((own, 8, chunk), F32),
                pltpu.VMEM((T, chunk), F32),
                pltpu.VMEM((2, chunk // 128, chunk, 128), BF16),
                DMA((own + 1,)), DMA((2,)), DMA((2,)), DMA((2,)), DMA((2,)), DMA, DMA, DMA((3,)), DMA((3,)), DMA((3,)), DMA((3,)),
            ],
            compiler_params=pltpu.CompilerParams(collective_id=0, has_side_effects=True, vmem_limit_bytes=48 * 1024 * 1024),
        )
        x_blocks = pos_loc.reshape(own, chunk, feat)
        pulled, sums, parts = call(pltpu.with_memory_space_constraint(x_blocks, pltpu.HBM),
                                   pltpu.with_memory_space_constraint(chg_loc.reshape(rows // 128, 128), pltpu.HBM))
        force, energy = pl.pallas_call(
            finish,
            out_shape=[jax.ShapeDtypeStruct((own, chunk, feat), F32), jax.ShapeDtypeStruct((1,), F32)],
            in_specs=[pl.BlockSpec(memory_space=pltpu.VMEM)] * 4,
            out_specs=[pl.BlockSpec(memory_space=pltpu.HBM), pl.BlockSpec(memory_space=pltpu.SMEM)],
            scratch_shapes=[pltpu.VMEM((own, chunk, feat), F32), DMA((own,))],
            compiler_params=pltpu.CompilerParams(vmem_limit_bytes=8 * 1024 * 1024),
        )(x_blocks, pulled, sums, parts)
        return force.reshape(rows, feat), energy

    return jax.shard_map(device_body, mesh=mesh, in_specs=(P(("sys", "row"), None), P(("sys", "row"))), out_specs=(P(("sys", "row"), None), P("sys")), check_vma=False)
```

```python
import functools
import math

import jax
import jax.numpy as jnp
from jax import lax
from jax.experimental import pallas as pl
from jax.experimental.pallas import tpu as pltpu
from jax.sharding import PartitionSpec as P

MESH = pl.DeviceIdType.MESH
T = 256
F32 = jnp.float32
BF16 = jnp.bfloat16
PIECE = 64


def split3(v):
    hi = v.astype(BF16).astype(F32)
    rest = v - hi
    mid = rest.astype(BF16).astype(F32)
    return hi, mid, rest - mid


def kernel(rows, feat, x_ref, q_ref, ft, rs, ebuf, xall, qall, aug, xt, qb, rhs, top, sign, sbuf, wbuf,
           lsem, xsend, xrecv, fsend, frecv, psend, precv, qsend, qrecv, esend, erecv):
    me = lax.axis_index("row")
    upper = me // 2
    partner = me + 1 - 2 * lax.rem(me, 2)
    third = (1 - upper) * (3 - me) + upper * (me - 2)
    last = third + 1 - 2 * lax.rem(third, 2)
    peers = (partner, third, last)
    chunk = 2 * T
    own = rows // chunk
    total = 4 * own
    lanes = chunk // 128
    scale = math.log2(math.e) / (2.0 * feat)

    local = [pltpu.make_async_copy(q_ref, qall.at[pl.ds(0, own * lanes)], lsem.at[own])]
    local += [pltpu.make_async_copy(x_ref.at[c], xall.at[c], lsem.at[c]) for c in range(own)]
    for copy in local:
        copy.start()
    barrier = pltpu.get_barrier_semaphore()
    for peer in peers:
        pl.semaphore_signal(barrier, inc=1, device_id={"row": peer}, device_id_type=MESH)

    def remote(src, dst, ssem, rsem, peer):
        return pltpu.make_async_remote_copy(src_ref=src, dst_ref=dst, send_sem=ssem, recv_sem=rsem,
                                            device_id={"row": peer}, device_id_type=MESH)

    q_copies = [remote(q_ref, qall.at[pl.ds((k + 1) * own * lanes, own * lanes)], qsend.at[k], qrecv.at[k], peer)
                for k, peer in enumerate(peers)]
    p_copy = remote(x_ref, xall.at[pl.ds(own, own)], psend, precv, partner)
    x_copies = [remote(x_ref.at[k], xall.at[2 * own + k], xsend.at[k], xrecv.at[k], third) for k in range(own)]
    f_copies = [remote(xall.at[2 * own + k], xall.at[3 * own + k], fsend.at[k], frecv.at[k], partner) for k in range(own)]

    row_id = lax.broadcasted_iota(jnp.int32, (8, chunk), 0)
    filler = jnp.zeros((120, chunk), F32)

    def norms(x_t):
        wide = x_t.astype(F32)
        return split3(jnp.sum(wide * wide, axis=0, keepdims=True))

    def q_row(g):
        return qall[pl.ds(g * lanes, lanes), :].reshape(1, chunk)

    def prepare(g, side):
        x_t = xall[g].T
        hi, mid, lo = norms(x_t)
        block = jnp.where(row_id == 0, hi, jnp.where(row_id == 1, mid, jnp.where(row_id == 2, lo, jnp.where(row_id < 6, 1.0, 0.0))))
        aug[side] = jnp.concatenate([block, filler], axis=0).astype(BF16).T
        qb[side] = jnp.broadcast_to(q_row(g), (128, chunk)).T
        for k in range(lanes):
            xt[side, k] = x_t[:, k * 128:(k + 1) * 128]

    def wide_load(ref, i):
        return jnp.concatenate([ref[i, k] for k in range(lanes)], axis=1)

    def first(g, side, h, t):
        lhs = jnp.concatenate([xall[g, pl.ds(h * T, T), :], aug[side, pl.ds(h * T, T), :]], axis=1)
        return jnp.dot(lhs, wide_load(rhs, t), preferred_element_type=F32)

    def weights(s, side, h, t, phase, masked, keep):
        top_t = top[t]
        acc = rs[phase, t]
        for p in range(T // PIECE):
            e = jnp.exp2(jnp.minimum(s(p).reshape(PIECE // 8, 8, chunk), top_t[None]) * scale).reshape(PIECE, chunk)
            rows_p = pl.ds(h * T + p * PIECE, PIECE)
            w = jnp.concatenate([qb[side, rows_p, :]] * lanes, axis=1) * e
            if masked:
                r = lax.broadcasted_iota(jnp.int32, (PIECE, chunk), 0) + (h * T + p * PIECE)
                w = jnp.where(r == lax.broadcasted_iota(jnp.int32, (PIECE, chunk), 1), 0.0, w)
            acc = acc + jnp.sum(w.reshape(PIECE // 8, 8, chunk), axis=0)
            w = w.astype(BF16)
            for j in range(lanes):
                wbuf[keep, j, rows_p, :] = w[:, j * 128:(j + 1) * 128]
        rs[phase, t] = acc

    def pull(side, t, keep):
        ft[t] += jnp.dot(wide_load(xt, side), wide_load(wbuf, keep), preferred_element_type=F32)

    def body(g, nxt, side, order, before, upcoming, phase, masked=False, hook=None):
        steps = [(k, h) for k in range(own) for h in range(2)]
        ready = lambda p: sbuf[pl.ds(p * PIECE, PIECE), :]
        for n, (k, h) in enumerate(steps):
            if n + 1 < len(steps):
                following = first(g, side, steps[n + 1][1], order[steps[n + 1][0]])
            if h == 0:
                if k == 0:
                    pull(1 - side, before, 1)
                else:
                    pull(side, order[k - 1], (k - 1) % 2)
            if n == 0 and nxt is not None:
                prepare(nxt, 1 - side)
            if n == 3 and hook is not None:
                hook()
            weights(ready, side, h, order[k], phase, masked and k == 0, k % 2)
            ready = lambda p, v=following: v[p * PIECE:(p + 1) * PIECE]
        if nxt is not None:
            sbuf[...] = first(nxt, 1 - side, 0, upcoming)

    pl.semaphore_wait(barrier, 3)
    for copy in x_copies:
        copy.start()
    for k in (1, 2, 0):
        q_copies[k].start()
    p_copy.start()
    rs[...] = jnp.zeros_like(rs)
    ft[...] = jnp.zeros_like(ft)
    wbuf[1] = jnp.zeros_like(wbuf[1])
    xt[1] = jnp.zeros_like(xt[1])
    local[0].wait()
    for c in range(own):
        local[1 + c].wait()
        q_c = q_row(c)
        sign[c] = jnp.broadcast_to(jnp.where(q_c < 0.0, -1.0, 1.0), (8, chunk))
        level = jnp.maximum(jnp.log2(jnp.abs(q_c)), -1000.0) * (1.0 / scale)
        top[c] = jnp.broadcast_to(level, (8, chunk))
        x_t = xall[c].T
        terms = [-1.0, -1.0, -1.0] + [v for v in split3(level - jnp.sum(jnp.square(x_t.astype(F32)), axis=0, keepdims=True))]
        block = jnp.zeros((8, chunk), F32)
        for k, v in enumerate(terms):
            block = jnp.where(row_id == k, v, block)
        block = jnp.concatenate([block, filler], axis=0).astype(BF16)
        double = x_t + x_t
        for k in range(lanes):
            rhs[c, k, pl.ds(0, feat), :] = double[:, k * 128:(k + 1) * 128]
            rhs[c, k, pl.ds(feat, 128), :] = block[:, k * 128:(k + 1) * 128]
    prepare(0, 0)
    sbuf[...] = first(0, 0, 0, 0)

    def total_of(phase):
        sums = (rs[phase, 0] * sign[0] + rs[phase, 1] * sign[1]) + (rs[phase, 2] * sign[2] + rs[phase, 3] * sign[3])
        return jnp.sum(jnp.sum(sums, axis=0, keepdims=True), axis=1, keepdims=True)
    e_copies = [remote(ebuf.at[me], ebuf.at[me], esend.at[k], erecv.at[k], peer) for k, peer in enumerate(peers)]

    def send_energy():
        for copy in e_copies:
            copy.start()

    x_id, f_id = 2 * own, 3 * own
    ids = list(range(2 * own)) + [x_id, x_id + 1, f_id, x_id + 2, f_id + 1, x_id + 3, f_id + 2, f_id + 3]
    fixed = list(range(own))
    before = own - 1
    for n, g in enumerate(ids):
        nxt = ids[n + 1] if n + 1 < len(ids) else None
        if nxt == own:
            q_copies[0].wait_recv()
            p_copy.wait_recv()
        if nxt == x_id:
            q_copies[1].wait_recv()
            q_copies[2].wait_recv()
        if nxt is not None and x_id <= nxt < f_id:
            x_copies[nxt - x_id].wait_recv()
            f_copies[nxt - x_id].start()
        if nxt is not None and nxt >= f_id:
            f_copies[nxt - f_id].wait_recv()
        order = fixed[n:] + fixed[:n] if n < own else fixed
        upcoming = n + 1 if n + 1 < own else 0
        body(g, nxt, n % 2, order, before, upcoming, 0 if g < x_id else 1 if g < f_id else 2, masked=n < own,
             hook=send_energy if g == f_id + 2 else None)
        before = order[-1]
        if g == f_id - 1:
            ebuf[me] = jnp.broadcast_to(0.5 * total_of(0) + total_of(1), (8, 128))
    pull(1, before, 1)

    for t in range(own):
        rs[0, t] = (rs[0, t] + rs[1, t]) + rs[2, t]
        rs[1, t] = sign[t]
    for copy in e_copies:
        copy.wait_recv()
    for copy in e_copies + q_copies + [p_copy] + x_copies + f_copies:
        copy.wait_send()


def finish(x_ref, ft, rs, ebuf, f_ref, e_ref, stage, value, sems):
    own, feat, chunk = ft.shape
    inv = 1.0 / feat
    energy = (ebuf[0] + ebuf[1]) + (ebuf[2] + ebuf[3])
    value[0] = jnp.max(energy[0:1, 0:1])
    copies = [pltpu.make_async_copy(value, e_ref, sems.at[own])]
    copies[0].start()
    for t in range(own):
        factor = rs[1, t, pl.ds(0, 1), :] * inv
        sums = jnp.sum(rs[0, t], axis=0, keepdims=True)
        stage[t] = ((sums * x_ref[t].T.astype(F32) - ft[t]) * factor).T
        copies.append(pltpu.make_async_copy(stage.at[t], f_ref.at[t], sems.at[t]))
        copies[-1].start()
    for copy in copies:
        copy.wait()


def solution(mesh):
    def device_body(pos_loc, chg_loc):
        rows, feat = pos_loc.shape
        chunk = 2 * T
        own = rows // chunk
        total = 4 * own
        DMA = pltpu.SemaphoreType.DMA
        call = pl.pallas_call(
            functools.partial(kernel, rows, feat),
            out_shape=[jax.ShapeDtypeStruct((own, feat, chunk), F32), jax.ShapeDtypeStruct((3, own, 8, chunk), F32),
                       jax.ShapeDtypeStruct((4, 8, 128), F32)],
            in_specs=[pl.BlockSpec(memory_space=pl.ANY)] * 2,
            out_specs=[pl.BlockSpec(memory_space=pltpu.VMEM)] * 3,
            scratch_shapes=[
                pltpu.VMEM((total, chunk, feat), BF16),
                pltpu.VMEM((4 * rows // 128, 128), F32),
                pltpu.VMEM((2, chunk, 128), BF16),
                pltpu.VMEM((2, chunk // 128, feat, 128), BF16),
                pltpu.VMEM((2, chunk, 128), F32),
                pltpu.VMEM((own, chunk // 128, 2 * 128, 128), BF16),
                pltpu.VMEM((own, 8, chunk), F32),
                pltpu.VMEM((own, 8, chunk), F32),
                pltpu.VMEM((T, chunk), F32),
                pltpu.VMEM((2, chunk // 128, chunk, 128), BF16),
                DMA((own + 1,)), DMA((own,)), DMA((own,)), DMA((own,)), DMA((own,)), DMA, DMA, DMA((3,)), DMA((3,)), DMA((3,)), DMA((3,)),
            ],
            compiler_params=pltpu.CompilerParams(collective_id=0, has_side_effects=True, vmem_limit_bytes=48 * 1024 * 1024),
        )
        x_blocks = pos_loc.reshape(own, chunk, feat)
        pulled, sums, parts = call(pltpu.with_memory_space_constraint(x_blocks, pltpu.HBM),
                                   pltpu.with_memory_space_constraint(chg_loc.reshape(rows // 128, 128), pltpu.HBM))
        force, energy = pl.pallas_call(
            finish,
            out_shape=[jax.ShapeDtypeStruct((own, chunk, feat), F32), jax.ShapeDtypeStruct((1,), F32)],
            in_specs=[pl.BlockSpec(memory_space=pltpu.VMEM)] * 4,
            out_specs=[pl.BlockSpec(memory_space=pltpu.HBM)] * 2,
            scratch_shapes=[pltpu.VMEM((own, chunk, feat), F32), pltpu.SMEM((1,), F32), DMA((own + 1,))],
            compiler_params=pltpu.CompilerParams(vmem_limit_bytes=8 * 1024 * 1024),
        )(x_blocks, pulled, sums, parts)
        return force.reshape(rows, feat), energy

    return jax.shard_map(device_body, mesh=mesh, in_specs=(P(("sys", "row"), None), P(("sys", "row"))), out_specs=(P(("sys", "row"), None), P("sys")), check_vma=False)
```

```python
import functools
import math

import jax
import jax.numpy as jnp
from jax import lax
from jax.experimental import pallas as pl
from jax.experimental.pallas import tpu as pltpu
from jax.sharding import PartitionSpec as P

MESH = pl.DeviceIdType.MESH
T = 256
F32 = jnp.float32
BF16 = jnp.bfloat16
PIECE = 64


def split3(v):
    hi = v.astype(BF16).astype(F32)
    rest = v - hi
    mid = rest.astype(BF16).astype(F32)
    return hi, mid, rest - mid


def kernel(rows, feat, x_ref, q_ref, ft, rs, ebuf, xall, qall, aug, xt, qb, rhs, top, sign, sbuf, wbuf,
           lsem, xsend, xrecv, fsend, frecv, psend, precv, qsend, qrecv, esend, erecv):
    me = lax.axis_index("row")
    upper = me // 2
    partner = me + 1 - 2 * lax.rem(me, 2)
    third = (1 - upper) * (3 - me) + upper * (me - 2)
    last = third + 1 - 2 * lax.rem(third, 2)
    peers = (partner, third, last)
    chunk = 2 * T
    own = rows // chunk
    total = 4 * own
    lanes = chunk // 128
    scale = math.log2(math.e) / (2.0 * feat)

    local = [pltpu.make_async_copy(q_ref, qall.at[pl.ds(0, own * lanes)], lsem.at[own])]
    local += [pltpu.make_async_copy(x_ref.at[c], xall.at[c], lsem.at[c]) for c in range(own)]
    for copy in local:
        copy.start()
    barrier = pltpu.get_barrier_semaphore()
    for peer in peers:
        pl.semaphore_signal(barrier, inc=1, device_id={"row": peer}, device_id_type=MESH)

    def remote(src, dst, ssem, rsem, peer):
        return pltpu.make_async_remote_copy(src_ref=src, dst_ref=dst, send_sem=ssem, recv_sem=rsem,
                                            device_id={"row": peer}, device_id_type=MESH)

    q_copies = [remote(q_ref, qall.at[pl.ds((k + 1) * own * lanes, own * lanes)], qsend.at[k], qrecv.at[k], peer)
                for k, peer in enumerate(peers)]
    p_copy = remote(x_ref, xall.at[pl.ds(own, own)], psend, precv, partner)
    x_copies = [remote(x_ref.at[k], xall.at[2 * own + k], xsend.at[k], xrecv.at[k], third) for k in range(own)]
    f_copies = [remote(xall.at[2 * own + k], xall.at[3 * own + k], fsend.at[k], frecv.at[k], partner) for k in range(own)]

    row_id = lax.broadcasted_iota(jnp.int32, (8, chunk), 0)
    filler = jnp.zeros((120, chunk), F32)

    def norms(x_t):
        wide = x_t.astype(F32)
        return split3(jnp.sum(wide * wide, axis=0, keepdims=True))

    def q_row(g):
        return qall[pl.ds(g * lanes, lanes), :].reshape(1, chunk)

    def prepare(g, side):
        x_t = xall[g].T
        hi, mid, lo = norms(x_t)
        block = jnp.where(row_id == 0, hi, jnp.where(row_id == 1, mid, jnp.where(row_id == 2, lo, jnp.where(row_id < 6, 1.0, 0.0))))
        aug[side] = jnp.concatenate([block, filler], axis=0).astype(BF16).T
        qb[side] = jnp.broadcast_to(q_row(g), (128, chunk)).T
        for k in range(lanes):
            xt[side, k] = x_t[:, k * 128:(k + 1) * 128]

    def wide_load(ref, i):
        return jnp.concatenate([ref[i, k] for k in range(lanes)], axis=1)

    def first(g, side, h, t):
        lhs = jnp.concatenate([xall[g, pl.ds(h * T, T), :], aug[side, pl.ds(h * T, T), :]], axis=1)
        return jnp.dot(lhs, wide_load(rhs, t), preferred_element_type=F32)

    def weights(s, side, h, t, phase, masked, keep):
        top_t = top[t]
        acc = rs[phase, t]
        for p in range(T // PIECE):
            e = jnp.exp2(jnp.minimum(s(p).reshape(PIECE // 8, 8, chunk), top_t[None]) * scale).reshape(PIECE, chunk)
            rows_p = pl.ds(h * T + p * PIECE, PIECE)
            w = jnp.concatenate([qb[side, rows_p, :]] * lanes, axis=1) * e
            if masked:
                r = lax.broadcasted_iota(jnp.int32, (PIECE, chunk), 0) + (h * T + p * PIECE)
                w = jnp.where(r == lax.broadcasted_iota(jnp.int32, (PIECE, chunk), 1), 0.0, w)
            acc = acc + jnp.sum(w.reshape(PIECE // 8, 8, chunk), axis=0)
            w = w.astype(BF16)
            for j in range(lanes):
                wbuf[keep, j, rows_p, :] = w[:, j * 128:(j + 1) * 128]
        rs[phase, t] = acc

    def pull(side, t, keep):
        ft[t] += jnp.dot(wide_load(xt, side), wide_load(wbuf, keep), preferred_element_type=F32)

    def body(g, nxt, side, order, before, upcoming, phase, masked=False, hook=None):
        steps = [(k, h) for k in range(own) for h in range(2)]
        ready = lambda p: sbuf[pl.ds(p * PIECE, PIECE), :]
        for n, (k, h) in enumerate(steps):
            if n + 1 < len(steps):
                following = first(g, side, steps[n + 1][1], order[steps[n + 1][0]])
            if h == 0:
                if k == 0:
                    pull(1 - side, before, 1)
                else:
                    pull(side, order[k - 1], (k - 1) % 2)
            if n == 0 and nxt is not None:
                prepare(nxt, 1 - side)
            if n == 3 and hook is not None:
                hook()
            weights(ready, side, h, order[k], phase, masked and k == 0, k % 2)
            ready = lambda p, v=following: v[p * PIECE:(p + 1) * PIECE]
        if nxt is not None:
            sbuf[...] = first(nxt, 1 - side, 0, upcoming)

    rs[...] = jnp.zeros_like(rs)
    ft[...] = jnp.zeros_like(ft)
    wbuf[1] = jnp.zeros_like(wbuf[1])
    xt[1] = jnp.zeros_like(xt[1])
    local[0].wait()
    for c in range(own):
        local[1 + c].wait()
        q_c = q_row(c)
        sign[c] = jnp.broadcast_to(jnp.where(q_c < 0.0, -1.0, 1.0), (8, chunk))
        level = jnp.maximum(jnp.log2(jnp.abs(q_c)), -1000.0) * (1.0 / scale)
        top[c] = jnp.broadcast_to(level, (8, chunk))
        x_t = xall[c].T
        terms = [-1.0, -1.0, -1.0] + [v for v in split3(level - jnp.sum(jnp.square(x_t.astype(F32)), axis=0, keepdims=True))]
        block = jnp.zeros((8, chunk), F32)
        for k, v in enumerate(terms):
            block = jnp.where(row_id == k, v, block)
        block = jnp.concatenate([block, filler], axis=0).astype(BF16)
        double = x_t + x_t
        for k in range(lanes):
            rhs[c, k, pl.ds(0, feat), :] = double[:, k * 128:(k + 1) * 128]
            rhs[c, k, pl.ds(feat, 128), :] = block[:, k * 128:(k + 1) * 128]
    pl.semaphore_wait(barrier, 3)
    for k in (1, 2, 0):
        q_copies[k].start()
    for copy in x_copies + [p_copy]:
        copy.start()
    prepare(0, 0)
    sbuf[...] = first(0, 0, 0, 0)

    def total_of(phase):
        sums = (rs[phase, 0] * sign[0] + rs[phase, 1] * sign[1]) + (rs[phase, 2] * sign[2] + rs[phase, 3] * sign[3])
        return jnp.sum(jnp.sum(sums, axis=0, keepdims=True), axis=1, keepdims=True)
    e_copies = [remote(ebuf.at[me], ebuf.at[me], esend.at[k], erecv.at[k], peer) for k, peer in enumerate(peers)]

    def send_energy():
        for copy in e_copies:
            copy.start()

    x_id, f_id = 2 * own, 3 * own
    ids = list(range(2 * own)) + [x_id, x_id + 1, f_id, x_id + 2, f_id + 1, x_id + 3, f_id + 2, f_id + 3]
    fixed = list(range(own))
    before = own - 1
    for n, g in enumerate(ids):
        nxt = ids[n + 1] if n + 1 < len(ids) else None
        if nxt == own:
            q_copies[0].wait_recv()
            p_copy.wait_recv()
        for k in {x_id: (0, 1), f_id: (2,), x_id + 3: (3,)}.get(nxt, ()):
            if k == 0:
                q_copies[1].wait_recv()
                q_copies[2].wait_recv()
            x_copies[k].wait_recv()
            f_copies[k].start()
        for k in {f_id: (0, 1), x_id + 3: (2,), f_id + 3: (3,)}.get(nxt, ()):
            f_copies[k].wait_recv()
        order = fixed[n:] + fixed[:n] if n < own else fixed
        upcoming = n + 1 if n + 1 < own else 0
        body(g, nxt, n % 2, order, before, upcoming, 0 if g < x_id else 1 if g < f_id else 2, masked=n < own,
             hook=send_energy if g == f_id + 2 else None)
        before = order[-1]
        if g == f_id - 1:
            ebuf[me] = jnp.broadcast_to(0.5 * total_of(0) + total_of(1), (8, 128))
    pull(1, before, 1)

    for t in range(own):
        rs[0, t] = (rs[0, t] + rs[1, t]) + rs[2, t]
        rs[1, t] = sign[t]
    for copy in e_copies:
        copy.wait_recv()
    for copy in e_copies + q_copies + [p_copy] + x_copies + f_copies:
        copy.wait_send()


def finish(x_ref, ft, rs, ebuf, f_ref, e_ref, stage, value, sems):
    own, feat, chunk = ft.shape
    inv = 1.0 / feat
    energy = (ebuf[0] + ebuf[1]) + (ebuf[2] + ebuf[3])
    value[0] = jnp.max(energy[0:1, 0:1])
    copies = [pltpu.make_async_copy(value, e_ref, sems.at[own])]
    copies[0].start()
    for t in range(own):
        factor = rs[1, t, pl.ds(0, 1), :] * inv
        sums = jnp.sum(rs[0, t], axis=0, keepdims=True)
        stage[t] = ((sums * x_ref[t].T.astype(F32) - ft[t]) * factor).T
        copies.append(pltpu.make_async_copy(stage.at[t], f_ref.at[t], sems.at[t]))
        copies[-1].start()
    for copy in copies:
        copy.wait()


def solution(mesh):
    def device_body(pos_loc, chg_loc):
        rows, feat = pos_loc.shape
        chunk = 2 * T
        own = rows // chunk
        total = 4 * own
        DMA = pltpu.SemaphoreType.DMA
        call = pl.pallas_call(
            functools.partial(kernel, rows, feat),
            out_shape=[jax.ShapeDtypeStruct((own, feat, chunk), F32), jax.ShapeDtypeStruct((3, own, 8, chunk), F32),
                       jax.ShapeDtypeStruct((4, 8, 128), F32)],
            in_specs=[pl.BlockSpec(memory_space=pl.ANY)] * 2,
            out_specs=[pl.BlockSpec(memory_space=pltpu.VMEM)] * 3,
            scratch_shapes=[
                pltpu.VMEM((total, chunk, feat), BF16),
                pltpu.VMEM((4 * rows // 128, 128), F32),
                pltpu.VMEM((2, chunk, 128), BF16),
                pltpu.VMEM((2, chunk // 128, feat, 128), BF16),
                pltpu.VMEM((2, chunk, 128), F32),
                pltpu.VMEM((own, chunk // 128, 2 * 128, 128), BF16),
                pltpu.VMEM((own, 8, chunk), F32),
                pltpu.VMEM((own, 8, chunk), F32),
                pltpu.VMEM((T, chunk), F32),
                pltpu.VMEM((2, chunk // 128, chunk, 128), BF16),
                DMA((own + 1,)), DMA((own,)), DMA((own,)), DMA((own,)), DMA((own,)), DMA, DMA, DMA((3,)), DMA((3,)), DMA((3,)), DMA((3,)),
            ],
            compiler_params=pltpu.CompilerParams(collective_id=0, has_side_effects=True, vmem_limit_bytes=48 * 1024 * 1024),
        )
        x_blocks = pos_loc.reshape(own, chunk, feat)
        pulled, sums, parts = call(pltpu.with_memory_space_constraint(x_blocks, pltpu.HBM),
                                   pltpu.with_memory_space_constraint(chg_loc.reshape(rows // 128, 128), pltpu.HBM))
        force, energy = pl.pallas_call(
            finish,
            out_shape=[jax.ShapeDtypeStruct((own, chunk, feat), F32), jax.ShapeDtypeStruct((1,), F32)],
            in_specs=[pl.BlockSpec(memory_space=pltpu.VMEM)] * 4,
            out_specs=[pl.BlockSpec(memory_space=pltpu.HBM)] * 2,
            scratch_shapes=[pltpu.VMEM((own, chunk, feat), F32), pltpu.SMEM((1,), F32), DMA((own + 1,))],
            compiler_params=pltpu.CompilerParams(vmem_limit_bytes=8 * 1024 * 1024),
        )(x_blocks, pulled, sums, parts)
        return force.reshape(rows, feat), energy

    return jax.shard_map(device_body, mesh=mesh, in_specs=(P(("sys", "row"), None), P(("sys", "row"))), out_specs=(P(("sys", "row"), None), P("sys")), check_vma=False)
```

```python
import functools
import math

import jax
import jax.numpy as jnp
from jax import lax
from jax.experimental import pallas as pl
from jax.experimental.pallas import tpu as pltpu
from jax.sharding import PartitionSpec as P

MESH = pl.DeviceIdType.MESH
T = 256
F32 = jnp.float32
BF16 = jnp.bfloat16
PIECE = 64


def split3(v):
    hi = v.astype(BF16).astype(F32)
    rest = v - hi
    mid = rest.astype(BF16).astype(F32)
    return hi, mid, rest - mid


def kernel(rows, feat, x_ref, q_ref, ft, rs, ebuf, xall, qall, aug, xt, qb, rhs, top, sign, xs, rcol, sbuf, wbuf,
           lsem, xsend, xrecv, fsend, frecv, psend, precv, qsend, qrecv, esend, erecv):
    me = lax.axis_index("row")
    upper = me // 2
    partner = me + 1 - 2 * lax.rem(me, 2)
    third = (1 - upper) * (3 - me) + upper * (me - 2)
    last = third + 1 - 2 * lax.rem(third, 2)
    peers = (partner, third, last)
    chunk = 2 * T
    own = rows // chunk
    total = 4 * own
    lanes = chunk // 128
    scale = math.log2(math.e) / (2.0 * feat)

    local = [pltpu.make_async_copy(q_ref, qall.at[pl.ds(0, own * lanes)], lsem.at[own])]
    local += [pltpu.make_async_copy(x_ref.at[c], xall.at[c], lsem.at[c]) for c in range(own)]
    for copy in local:
        copy.start()
    barrier = pltpu.get_barrier_semaphore()
    for peer in peers:
        pl.semaphore_signal(barrier, inc=1, device_id={"row": peer}, device_id_type=MESH)

    def remote(src, dst, ssem, rsem, peer):
        return pltpu.make_async_remote_copy(src_ref=src, dst_ref=dst, send_sem=ssem, recv_sem=rsem,
                                            device_id={"row": peer}, device_id_type=MESH)

    q_copies = [remote(q_ref, qall.at[pl.ds((k + 1) * own * lanes, own * lanes)], qsend.at[k], qrecv.at[k], peer)
                for k, peer in enumerate(peers)]
    p_copy = remote(x_ref, xall.at[pl.ds(own, own)], psend, precv, partner)
    x_copies = [remote(x_ref.at[k], xall.at[2 * own + k], xsend.at[k], xrecv.at[k], third) for k in range(own)]
    f_copies = [remote(xall.at[2 * own + k], xall.at[3 * own + k], fsend.at[k], frecv.at[k], partner) for k in range(own)]

    row_id = lax.broadcasted_iota(jnp.int32, (8, chunk), 0)
    filler = jnp.zeros((120, chunk), F32)

    def norms(x_t):
        wide = x_t.astype(F32)
        return split3(jnp.sum(wide * wide, axis=0, keepdims=True))

    def q_row(g):
        return qall[pl.ds(g * lanes, lanes), :].reshape(1, chunk)

    def prepare(g, side):
        x_t = xall[g].T
        hi, mid, lo = norms(x_t)
        block = jnp.where(row_id == 0, hi, jnp.where(row_id == 1, mid, jnp.where(row_id == 2, lo, jnp.where(row_id < 6, 1.0, 0.0))))
        aug[side] = jnp.concatenate([block, filler], axis=0).astype(BF16).T
        qb[side] = jnp.broadcast_to(q_row(g), (128, chunk)).T
        for k in range(lanes):
            xt[side, k] = x_t[:, k * 128:(k + 1) * 128]

    def wide_load(ref, i):
        return jnp.concatenate([ref[i, k] for k in range(lanes)], axis=1)

    def first(g, side, h, t):
        lhs = jnp.concatenate([xall[g, pl.ds(h * T, T), :], aug[side, pl.ds(h * T, T), :]], axis=1)
        return jnp.dot(lhs, wide_load(rhs, t), preferred_element_type=F32)

    def weights(s, side, h, t, phase, masked, keep, row):
        top_t = top[t]
        acc = rs[phase, t]
        for p in range(T // PIECE):
            e = jnp.exp2(jnp.minimum(s(p).reshape(PIECE // 8, 8, chunk), top_t[None]) * scale).reshape(PIECE, chunk)
            rows_p = pl.ds(h * T + p * PIECE, PIECE)
            w = jnp.concatenate([qb[side, rows_p, :]] * lanes, axis=1) * e
            if masked:
                r = lax.broadcasted_iota(jnp.int32, (PIECE, chunk), 0) + (h * T + p * PIECE)
                w = jnp.where(r == lax.broadcasted_iota(jnp.int32, (PIECE, chunk), 1), 0.0, w)
            acc = acc + jnp.sum(w.reshape(PIECE // 8, 8, chunk), axis=0)
            if row is not None:
                ws = (w.reshape(PIECE // 8, 8, chunk) * sign[t][None]).reshape(PIECE, chunk)
                along = (ws[:, 0:128] + ws[:, 128:256]) + (ws[:, 256:384] + ws[:, 384:512])
                rcol[row, rows_p, :] = along if t == row + 1 else rcol[row, rows_p, :] + along
            w = w.astype(BF16)
            for j in range(lanes):
                wbuf[keep, j, rows_p, :] = w[:, j * 128:(j + 1) * 128]
        rs[phase, t] = acc

    def pull(side, t, keep, row):
        w = wide_load(wbuf, keep)
        ft[t] += jnp.dot(wide_load(xt, side), w, preferred_element_type=F32)
        if row is not None:
            back = lax.dot_general(wide_load(xs, t), w, (((1,), (1,)), ((), ())), preferred_element_type=F32)
            ft[row] += (back.reshape(feat // 8, 8, chunk) * sign[row][None]).reshape(feat, chunk)

    def row_sums():
        for c in range(own - 1):
            rs[0, c] += jnp.sum(rcol[c].T.reshape(16, 8, chunk), axis=0) * sign[c]

    def body(g, nxt, side, groups, previous, upcoming, hooks):
        steps = [(k, h) for k in range(len(groups)) for h in range(2)]
        ready = lambda p: sbuf[pl.ds(p * PIECE, PIECE), :]
        for n, (k, h) in enumerate(steps):
            t, phase, masked, row, keep = groups[k]
            if n + 1 < len(steps):
                following = first(g, side, steps[n + 1][1], groups[steps[n + 1][0]][0])
            if h == 0 and previous is not None:
                pull(*previous)
            if n == 0 and nxt is not None:
                prepare(nxt, 1 - side)
            if n in hooks:
                hooks[n]()
            weights(ready, side, h, t, phase, masked, keep, row)
            ready = lambda p, v=following: v[p * PIECE:(p + 1) * PIECE]
            if h == 1:
                previous = (side, t, keep, row)
        if nxt is not None:
            sbuf[...] = first(nxt, 1 - side, 0, upcoming)
        return previous

    rs[...] = jnp.zeros_like(rs)
    ft[...] = jnp.zeros_like(ft)
    local[0].wait()
    for c in range(own):
        local[1 + c].wait()
        q_c = q_row(c)
        sign[c] = jnp.broadcast_to(jnp.where(q_c < 0.0, -1.0, 1.0), (8, chunk))
        level = jnp.maximum(jnp.log2(jnp.abs(q_c)), -1000.0) * (1.0 / scale)
        top[c] = jnp.broadcast_to(level, (8, chunk))
        x_t = xall[c].T
        terms = [-1.0, -1.0, -1.0] + [v for v in split3(level - jnp.sum(jnp.square(x_t.astype(F32)), axis=0, keepdims=True))]
        block = jnp.zeros((8, chunk), F32)
        for k, v in enumerate(terms):
            block = jnp.where(row_id == k, v, block)
        block = jnp.concatenate([block, filler], axis=0).astype(BF16)
        double = x_t + x_t
        signed = x_t * jnp.where(q_c < 0.0, -1.0, 1.0).astype(BF16)
        for k in range(lanes):
            rhs[c, k, pl.ds(0, feat), :] = double[:, k * 128:(k + 1) * 128]
            xs[c, k] = signed[:, k * 128:(k + 1) * 128]
            rhs[c, k, pl.ds(feat, 128), :] = block[:, k * 128:(k + 1) * 128]
    pl.semaphore_wait(barrier, 3)
    for k in (1, 2, 0):
        q_copies[k].start()
    for copy in x_copies + [p_copy]:
        copy.start()
    prepare(0, 0)
    sbuf[...] = first(0, 0, 0, 0)

    def total_of(phase):
        sums = (rs[phase, 0] * sign[0] + rs[phase, 1] * sign[1]) + (rs[phase, 2] * sign[2] + rs[phase, 3] * sign[3])
        return jnp.sum(jnp.sum(sums, axis=0, keepdims=True), axis=1, keepdims=True)
    e_copies = [remote(ebuf.at[me], ebuf.at[me], esend.at[k], erecv.at[k], peer) for k, peer in enumerate(peers)]

    def send_energy():
        for copy in e_copies:
            copy.start()

    def close_energy():
        ebuf[me] = jnp.broadcast_to(0.5 * total_of(0) + total_of(1), (8, 128))

    x_id, f_id, end = 2 * own, 3 * own, own - 1
    ids = list(range(2 * own)) + [x_id, x_id + 1, f_id, f_id + 1, x_id + 2, f_id + 2, x_id + 3, f_id + 3]
    x_waits = {x_id: (0, 1), x_id + 2: (2,), x_id + 3: (3,)}
    f_waits = {f_id: (0, 1), f_id + 2: (2,), f_id + 3: (3,)}

    def phase_of(g, t):
        if g < x_id:
            return 0
        if g < x_id + end or (t == end and g < f_id + end):
            return 1
        return 2

    count, previous = 0, None
    for n, g in enumerate(ids):
        nxt = ids[n + 1] if n + 1 < len(ids) else None
        if nxt == own:
            q_copies[0].wait_recv()
            p_copy.wait_recv()
        if nxt == x_id:
            q_copies[1].wait_recv()
            q_copies[2].wait_recv()
        for k in x_waits.get(nxt, ()):
            x_copies[k].wait_recv()
            f_copies[k].start()
        for k in f_waits.get(nxt, ()):
            f_copies[k].wait_recv()
        first_t = lambda m, i: m if m < own else end if i == x_id + end else 0
        hooks = {own: {2: row_sums}, 2 * own + 6: {2: close_energy, 5: send_energy}}.get(n, {})
        groups = []
        for k in range(own - n if n < own else own):
            t = n + k if n < own else (first_t(n, g) + k) % own
            groups.append((t, phase_of(g, t), t == n and n < own, n if n < own and t > n else None, count % 2))
            count += 1
        previous = body(g, nxt, n % 2, groups, previous, first_t(n + 1, nxt), hooks)
    pull(*previous)

    for t in range(own):
        rs[0, t] = (rs[0, t] + rs[1, t]) + rs[2, t]
        rs[1, t] = sign[t]
    for copy in e_copies:
        copy.wait_recv()
    for copy in e_copies + q_copies + [p_copy] + x_copies + f_copies:
        copy.wait_send()


def finish(x_ref, ft, rs, ebuf, f_ref, e_ref, stage, value, sems):
    own, feat, chunk = ft.shape
    inv = 1.0 / feat
    energy = (ebuf[0] + ebuf[1]) + (ebuf[2] + ebuf[3])
    value[0] = jnp.max(energy[0:1, 0:1])
    copies = [pltpu.make_async_copy(value, e_ref, sems.at[own])]
    copies[0].start()
    for t in range(own):
        factor = rs[1, t, pl.ds(0, 1), :] * inv
        sums = jnp.sum(rs[0, t], axis=0, keepdims=True)
        stage[t] = ((sums * x_ref[t].T.astype(F32) - ft[t]) * factor).T
        copies.append(pltpu.make_async_copy(stage.at[t], f_ref.at[t], sems.at[t]))
        copies[-1].start()
    for copy in copies:
        copy.wait()


def solution(mesh):
    def device_body(pos_loc, chg_loc):
        rows, feat = pos_loc.shape
        chunk = 2 * T
        own = rows // chunk
        total = 4 * own
        DMA = pltpu.SemaphoreType.DMA
        call = pl.pallas_call(
            functools.partial(kernel, rows, feat),
            out_shape=[jax.ShapeDtypeStruct((own, feat, chunk), F32), jax.ShapeDtypeStruct((3, own, 8, chunk), F32),
                       jax.ShapeDtypeStruct((4, 8, 128), F32)],
            in_specs=[pl.BlockSpec(memory_space=pl.ANY)] * 2,
            out_specs=[pl.BlockSpec(memory_space=pltpu.VMEM)] * 3,
            scratch_shapes=[
                pltpu.VMEM((total, chunk, feat), BF16),
                pltpu.VMEM((4 * rows // 128, 128), F32),
                pltpu.VMEM((2, chunk, 128), BF16),
                pltpu.VMEM((2, chunk // 128, feat, 128), BF16),
                pltpu.VMEM((2, chunk, 128), F32),
                pltpu.VMEM((own, chunk // 128, 2 * 128, 128), BF16),
                pltpu.VMEM((own, 8, chunk), F32),
                pltpu.VMEM((own, 8, chunk), F32),
                pltpu.VMEM((own, chunk // 128, feat, 128), BF16),
                pltpu.VMEM((own - 1, chunk, 128), F32),
                pltpu.VMEM((T, chunk), F32),
                pltpu.VMEM((2, chunk // 128, chunk, 128), BF16),
                DMA((own + 1,)), DMA((own,)), DMA((own,)), DMA((own,)), DMA((own,)), DMA, DMA, DMA((3,)), DMA((3,)), DMA((3,)), DMA((3,)),
            ],
            compiler_params=pltpu.CompilerParams(collective_id=0, has_side_effects=True, vmem_limit_bytes=48 * 1024 * 1024),
        )
        x_blocks = pos_loc.reshape(own, chunk, feat)
        pulled, sums, parts = call(pltpu.with_memory_space_constraint(x_blocks, pltpu.HBM),
                                   pltpu.with_memory_space_constraint(chg_loc.reshape(rows // 128, 128), pltpu.HBM))
        force, energy = pl.pallas_call(
            finish,
            out_shape=[jax.ShapeDtypeStruct((own, chunk, feat), F32), jax.ShapeDtypeStruct((1,), F32)],
            in_specs=[pl.BlockSpec(memory_space=pltpu.VMEM)] * 4,
            out_specs=[pl.BlockSpec(memory_space=pltpu.HBM)] * 2,
            scratch_shapes=[pltpu.VMEM((own, chunk, feat), F32), pltpu.SMEM((1,), F32), DMA((own + 1,))],
            compiler_params=pltpu.CompilerParams(vmem_limit_bytes=8 * 1024 * 1024),
        )(x_blocks, pulled, sums, parts)
        return force.reshape(rows, feat), energy

    return jax.shard_map(device_body, mesh=mesh, in_specs=(P(("sys", "row"), None), P(("sys", "row"))), out_specs=(P(("sys", "row"), None), P("sys")), check_vma=False)
```

```python
import functools
import math

import jax
import jax.numpy as jnp
from jax import lax
from jax.experimental import pallas as pl
from jax.experimental.pallas import tpu as pltpu
from jax.sharding import PartitionSpec as P

MESH = pl.DeviceIdType.MESH
T = 256
F32 = jnp.float32
BF16 = jnp.bfloat16
PIECE = 64


def split3(v):
    hi = v.astype(BF16).astype(F32)
    rest = v - hi
    mid = rest.astype(BF16).astype(F32)
    return hi, mid, rest - mid


def kernel(rows, feat, x_ref, q_ref, ft, rs, ebuf, xall, qall, aug, xt, qb, rhs, top, sign, xs, rcol, sbuf, wbuf,
           lsem, xsend, xrecv, fsend, frecv, psend, precv, qsend, qrecv, esend, erecv):
    me = lax.axis_index("row")
    upper = me // 2
    partner = me + 1 - 2 * lax.rem(me, 2)
    third = (1 - upper) * (3 - me) + upper * (me - 2)
    last = third + 1 - 2 * lax.rem(third, 2)
    peers = (partner, third, last)
    chunk = 2 * T
    own = rows // chunk
    total = 4 * own
    lanes = chunk // 128
    scale = math.log2(math.e) / (2.0 * feat)

    local = [pltpu.make_async_copy(q_ref, qall.at[pl.ds(0, own * lanes)], lsem.at[own])]
    local += [pltpu.make_async_copy(x_ref.at[c], xall.at[c], lsem.at[c]) for c in range(own)]
    for copy in local:
        copy.start()
    barrier = pltpu.get_barrier_semaphore()
    for peer in peers:
        pl.semaphore_signal(barrier, inc=1, device_id={"row": peer}, device_id_type=MESH)

    def remote(src, dst, ssem, rsem, peer):
        return pltpu.make_async_remote_copy(src_ref=src, dst_ref=dst, send_sem=ssem, recv_sem=rsem,
                                            device_id={"row": peer}, device_id_type=MESH)

    q_copies = [remote(q_ref, qall.at[pl.ds((k + 1) * own * lanes, own * lanes)], qsend.at[k], qrecv.at[k], peer)
                for k, peer in enumerate(peers)]
    p_copy = remote(x_ref, xall.at[pl.ds(own, own)], psend, precv, partner)
    x_copies = [remote(x_ref.at[k], xall.at[2 * own + k], xsend.at[k], xrecv.at[k], third) for k in range(own)]
    f_copies = [remote(xall.at[2 * own + k], xall.at[3 * own + k], fsend.at[k], frecv.at[k], partner) for k in range(own)]

    row_id = lax.broadcasted_iota(jnp.int32, (8, chunk), 0)
    filler = jnp.zeros((120, chunk), F32)

    def norms(x_t):
        wide = x_t.astype(F32)
        return split3(jnp.sum(wide * wide, axis=0, keepdims=True))

    def q_row(g):
        return qall[pl.ds(g * lanes, lanes), :].reshape(1, chunk)

    def prepare(g, side):
        x_t = xall[g].T
        hi, mid, lo = norms(x_t)
        block = jnp.where(row_id == 0, hi, jnp.where(row_id == 1, mid, jnp.where(row_id == 2, lo, jnp.where(row_id < 6, 1.0, 0.0))))
        aug[side] = jnp.concatenate([block, filler], axis=0).astype(BF16).T
        qb[side] = jnp.broadcast_to(q_row(g), (128, chunk)).T
        for k in range(lanes):
            xt[side, k] = x_t[:, k * 128:(k + 1) * 128]

    def wide_load(ref, i):
        return jnp.concatenate([ref[i, k] for k in range(lanes)], axis=1)

    def first(g, side, h, t):
        lhs = jnp.concatenate([xall[g, pl.ds(h * T, T), :], aug[side, pl.ds(h * T, T), :]], axis=1)
        return jnp.dot(lhs, wide_load(rhs, t), preferred_element_type=F32)

    def weights(s, side, h, t, phase, masked, keep, row):
        top_t = top[t]
        acc = rs[phase, t]
        for p in range(T // PIECE):
            e = jnp.exp2(jnp.minimum(s(p).reshape(PIECE // 8, 8, chunk), top_t[None]) * scale).reshape(PIECE, chunk)
            rows_p = pl.ds(h * T + p * PIECE, PIECE)
            w = jnp.concatenate([qb[side, rows_p, :]] * lanes, axis=1) * e
            if masked:
                r = lax.broadcasted_iota(jnp.int32, (PIECE, chunk), 0) + (h * T + p * PIECE)
                w = jnp.where(r == lax.broadcasted_iota(jnp.int32, (PIECE, chunk), 1), 0.0, w)
            acc = acc + jnp.sum(w.reshape(PIECE // 8, 8, chunk), axis=0)
            if row is not None:
                ws = (w.reshape(PIECE // 8, 8, chunk) * sign[t][None]).reshape(PIECE, chunk)
                along = (ws[:, 0:128] + ws[:, 128:256]) + (ws[:, 256:384] + ws[:, 384:512])
                rcol[row, rows_p, :] = along if t == row + 1 else rcol[row, rows_p, :] + along
            w = w.astype(BF16)
            for j in range(lanes):
                wbuf[keep, j, rows_p, :] = w[:, j * 128:(j + 1) * 128]
        rs[phase, t] = acc

    def pull(side, t, keep, row):
        w = wide_load(wbuf, keep)
        ft[t] += jnp.dot(wide_load(xt, side), w, preferred_element_type=F32)
        if row is not None:
            back = lax.dot_general(wide_load(xs, t), w, (((1,), (1,)), ((), ())), preferred_element_type=F32)
            ft[row] += (back.reshape(feat // 8, 8, chunk) * sign[row][None]).reshape(feat, chunk)

    def row_sums():
        for c in range(own - 1):
            rs[0, c] += jnp.sum(rcol[c].T.reshape(16, 8, chunk), axis=0) * sign[c]

    def body(g, nxt, side, groups, previous, upcoming, hooks, arrive):
        steps = [(k, h) for k in range(len(groups)) for h in range(2)]
        ready = lambda p: sbuf[pl.ds(p * PIECE, PIECE), :]
        for n, (k, h) in enumerate(steps):
            t, phase, masked, row, keep = groups[k]
            if n == 1 and arrive is not None:
                arrive()
            if n + 1 < len(steps):
                following = first(g, side, steps[n + 1][1], groups[steps[n + 1][0]][0])
            if h == 0 and previous is not None:
                pull(*previous)
            if n == (0 if arrive is None else 1) and nxt is not None:
                prepare(nxt, 1 - side)
            if n in hooks:
                hooks[n]()
            weights(ready, side, h, t, phase, masked, keep, row)
            ready = lambda p, v=following: v[p * PIECE:(p + 1) * PIECE]
            if h == 1:
                previous = (side, t, keep, row)
        if nxt is not None:
            sbuf[...] = first(nxt, 1 - side, 0, upcoming)
        return previous

    rs[...] = jnp.zeros_like(rs)
    ft[...] = jnp.zeros_like(ft)
    local[0].wait()
    for c in range(own):
        local[1 + c].wait()
        q_c = q_row(c)
        sign[c] = jnp.broadcast_to(jnp.where(q_c < 0.0, -1.0, 1.0), (8, chunk))
        level = jnp.maximum(jnp.log2(jnp.abs(q_c)), -1000.0) * (1.0 / scale)
        top[c] = jnp.broadcast_to(level, (8, chunk))
        x_t = xall[c].T
        terms = [-1.0, -1.0, -1.0] + [v for v in split3(level - jnp.sum(jnp.square(x_t.astype(F32)), axis=0, keepdims=True))]
        block = jnp.zeros((8, chunk), F32)
        for k, v in enumerate(terms):
            block = jnp.where(row_id == k, v, block)
        block = jnp.concatenate([block, filler], axis=0).astype(BF16)
        double = x_t + x_t
        signed = x_t * jnp.where(q_c < 0.0, -1.0, 1.0).astype(BF16)
        for k in range(lanes):
            rhs[c, k, pl.ds(0, feat), :] = double[:, k * 128:(k + 1) * 128]
            xs[c, k] = signed[:, k * 128:(k + 1) * 128]
            rhs[c, k, pl.ds(feat, 128), :] = block[:, k * 128:(k + 1) * 128]
    pl.semaphore_wait(barrier, 3)
    for k in (1, 2, 0):
        q_copies[k].start()
    for copy in x_copies[:own // 2] + [p_copy]:
        copy.start()
    prepare(0, 0)
    sbuf[...] = first(0, 0, 0, 0)

    def total_of(phase):
        sums = (rs[phase, 0] * sign[0] + rs[phase, 1] * sign[1]) + (rs[phase, 2] * sign[2] + rs[phase, 3] * sign[3])
        return jnp.sum(jnp.sum(sums, axis=0, keepdims=True), axis=1, keepdims=True)
    e_copies = [remote(ebuf.at[me], ebuf.at[me], esend.at[k], erecv.at[k], peer) for k, peer in enumerate(peers)]

    def send_energy():
        for copy in e_copies:
            copy.start()

    def close_energy():
        ebuf[me] = jnp.broadcast_to(0.5 * total_of(0) + total_of(1), (8, 128))

    x_id, f_id, end = 2 * own, 3 * own, own - 1
    ids = list(range(2 * own)) + [x_id, x_id + 1, f_id, f_id + 1, x_id + 2, f_id + 2, x_id + 3, f_id + 3]
    x_waits = {x_id: (0,), x_id + 1: (1,), x_id + 2: (2,), x_id + 3: (3,)}
    f_waits = {f_id: (0, 1), f_id + 2: (2,), f_id + 3: (3,)}

    def arrivals(nxt):
        if nxt == own:
            q_copies[0].wait_recv()
            p_copy.wait_recv()
            for copy in x_copies[own // 2:]:
                copy.start()
        if nxt == x_id:
            q_copies[1].wait_recv()
            q_copies[2].wait_recv()
        for k in x_waits.get(nxt, ()):
            x_copies[k].wait_recv()
            f_copies[k].start()
        for k in f_waits.get(nxt, ()):
            f_copies[k].wait_recv()

    def phase_of(g, t):
        if g < x_id:
            return 0
        if g < x_id + end or (t == end and g < f_id + end):
            return 1
        return 2

    count, previous = 0, None
    for n, g in enumerate(ids):
        nxt = ids[n + 1] if n + 1 < len(ids) else None
        awaited = nxt == own or nxt in x_waits or nxt in f_waits
        first_t = lambda m, i: m if m < own else end if i == x_id + end else 0
        hooks = {own: {2: row_sums}, 2 * own + 6: {2: close_energy, 5: send_energy}}.get(n, {})
        groups = []
        for k in range(own - n if n < own else own):
            t = n + k if n < own else (first_t(n, g) + k) % own
            groups.append((t, phase_of(g, t), t == n and n < own, n if n < own and t > n else None, count % 2))
            count += 1
        previous = body(g, nxt, n % 2, groups, previous, first_t(n + 1, nxt), hooks,
                        functools.partial(arrivals, nxt) if awaited else None)
    pull(*previous)

    for t in range(own):
        rs[0, t] = (rs[0, t] + rs[1, t]) + rs[2, t]
        rs[1, t] = sign[t]
    for copy in e_copies:
        copy.wait_recv()
    for copy in e_copies + q_copies + [p_copy] + x_copies + f_copies:
        copy.wait_send()


def finish(x_ref, ft, rs, ebuf, f_ref, e_ref, stage, value, sems):
    own, feat, chunk = ft.shape
    inv = 1.0 / feat
    energy = (ebuf[0] + ebuf[1]) + (ebuf[2] + ebuf[3])
    value[0] = jnp.max(energy[0:1, 0:1])
    copies = [pltpu.make_async_copy(value, e_ref, sems.at[own])]
    copies[0].start()
    for t in range(own):
        factor = rs[1, t, pl.ds(0, 1), :] * inv
        sums = jnp.sum(rs[0, t], axis=0, keepdims=True)
        stage[t] = ((sums * x_ref[t].T.astype(F32) - ft[t]) * factor).T
        copies.append(pltpu.make_async_copy(stage.at[t], f_ref.at[t], sems.at[t]))
        copies[-1].start()
    for copy in copies:
        copy.wait()


def solution(mesh):
    def device_body(pos_loc, chg_loc):
        rows, feat = pos_loc.shape
        chunk = 2 * T
        own = rows // chunk
        total = 4 * own
        DMA = pltpu.SemaphoreType.DMA
        call = pl.pallas_call(
            functools.partial(kernel, rows, feat),
            out_shape=[jax.ShapeDtypeStruct((own, feat, chunk), F32), jax.ShapeDtypeStruct((3, own, 8, chunk), F32),
                       jax.ShapeDtypeStruct((4, 8, 128), F32)],
            in_specs=[pl.BlockSpec(memory_space=pl.ANY)] * 2,
            out_specs=[pl.BlockSpec(memory_space=pltpu.VMEM)] * 3,
            scratch_shapes=[
                pltpu.VMEM((total, chunk, feat), BF16),
                pltpu.VMEM((4 * rows // 128, 128), F32),
                pltpu.VMEM((2, chunk, 128), BF16),
                pltpu.VMEM((2, chunk // 128, feat, 128), BF16),
                pltpu.VMEM((2, chunk, 128), F32),
                pltpu.VMEM((own, chunk // 128, 2 * 128, 128), BF16),
                pltpu.VMEM((own, 8, chunk), F32),
                pltpu.VMEM((own, 8, chunk), F32),
                pltpu.VMEM((own, chunk // 128, feat, 128), BF16),
                pltpu.VMEM((own - 1, chunk, 128), F32),
                pltpu.VMEM((T, chunk), F32),
                pltpu.VMEM((2, chunk // 128, chunk, 128), BF16),
                DMA((own + 1,)), DMA((own,)), DMA((own,)), DMA((own,)), DMA((own,)), DMA, DMA, DMA((3,)), DMA((3,)), DMA((3,)), DMA((3,)),
            ],
            compiler_params=pltpu.CompilerParams(collective_id=0, has_side_effects=True, vmem_limit_bytes=48 * 1024 * 1024),
        )
        x_blocks = pos_loc.reshape(own, chunk, feat)
        pulled, sums, parts = call(pltpu.with_memory_space_constraint(x_blocks, pltpu.HBM),
                                   pltpu.with_memory_space_constraint(chg_loc.reshape(rows // 128, 128), pltpu.HBM))
        force, energy = pl.pallas_call(
            finish,
            out_shape=[jax.ShapeDtypeStruct((own, chunk, feat), F32), jax.ShapeDtypeStruct((1,), F32)],
            in_specs=[pl.BlockSpec(memory_space=pltpu.VMEM)] * 4,
            out_specs=[pl.BlockSpec(memory_space=pltpu.HBM)] * 2,
            scratch_shapes=[pltpu.VMEM((own, chunk, feat), F32), pltpu.SMEM((1,), F32), DMA((own + 1,))],
            compiler_params=pltpu.CompilerParams(vmem_limit_bytes=8 * 1024 * 1024),
        )(x_blocks, pulled, sums, parts)
        return force.reshape(rows, feat), energy

    return jax.shard_map(device_body, mesh=mesh, in_specs=(P(("sys", "row"), None), P(("sys", "row"))), out_specs=(P(("sys", "row"), None), P("sys")), check_vma=False)
```

```python
import functools
import math

import jax
import jax.numpy as jnp
from jax import lax
from jax.experimental import pallas as pl
from jax.experimental.pallas import tpu as pltpu
from jax.sharding import PartitionSpec as P

MESH = pl.DeviceIdType.MESH
T = 256
F32 = jnp.float32
BF16 = jnp.bfloat16
PIECE = 64


def split3(v):
    hi = v.astype(BF16).astype(F32)
    rest = v - hi
    mid = rest.astype(BF16).astype(F32)
    return hi, mid, rest - mid


def kernel(rows, feat, x_ref, q_ref, ft, rs, ebuf, stage, xall, qall, aug, xt, qb, rhs, top, sign, xs, rcol, sbuf, wbuf,
           lsem, xsend, xrecv, fsend, frecv, psend, precv, qsend, qrecv, esend, erecv):
    me = lax.axis_index("row")
    upper = me // 2
    partner = me + 1 - 2 * lax.rem(me, 2)
    third = (1 - upper) * (3 - me) + upper * (me - 2)
    last = third + 1 - 2 * lax.rem(third, 2)
    peers = (partner, third, last)
    chunk = 2 * T
    own = rows // chunk
    total = 4 * own
    lanes = chunk // 128
    scale = math.log2(math.e) / (2.0 * feat)

    local = [pltpu.make_async_copy(q_ref, qall.at[pl.ds(0, own * lanes)], lsem.at[own])]
    local += [pltpu.make_async_copy(x_ref.at[c], xall.at[c], lsem.at[c]) for c in range(own)]
    for copy in local:
        copy.start()
    barrier = pltpu.get_barrier_semaphore()
    for peer in peers:
        pl.semaphore_signal(barrier, inc=1, device_id={"row": peer}, device_id_type=MESH)

    def remote(src, dst, ssem, rsem, peer):
        return pltpu.make_async_remote_copy(src_ref=src, dst_ref=dst, send_sem=ssem, recv_sem=rsem,
                                            device_id={"row": peer}, device_id_type=MESH)

    q_copies = [remote(q_ref, qall.at[pl.ds((k + 1) * own * lanes, own * lanes)], qsend.at[k], qrecv.at[k], peer)
                for k, peer in enumerate(peers)]
    p_copy = remote(xall.at[pl.ds(0, own)], xall.at[pl.ds(own, own)], psend, precv, partner)
    x_copies = [remote(xall.at[k], xall.at[2 * own + k], xsend.at[k], xrecv.at[k], third) for k in range(own)]
    f_copies = [remote(xall.at[2 * own + k], xall.at[3 * own + k], fsend.at[k], frecv.at[k], partner) for k in range(own)]

    row_id = lax.broadcasted_iota(jnp.int32, (8, chunk), 0)
    filler = jnp.zeros((120, chunk), F32)

    def norms(x_t):
        wide = x_t.astype(F32)
        return split3(jnp.sum(wide * wide, axis=0, keepdims=True))

    def q_row(g):
        return qall[pl.ds(g * lanes, lanes), :].reshape(1, chunk)

    def prepare(g, side):
        x_t = xall[g].T
        hi, mid, lo = norms(x_t)
        block = jnp.where(row_id == 0, hi, jnp.where(row_id == 1, mid, jnp.where(row_id == 2, lo, jnp.where(row_id < 6, 1.0, 0.0))))
        aug[side] = jnp.concatenate([block, filler], axis=0).astype(BF16).T
        qb[side] = jnp.broadcast_to(q_row(g), (128, chunk)).T
        for k in range(lanes):
            xt[side, k] = x_t[:, k * 128:(k + 1) * 128]

    def wide_load(ref, i):
        return jnp.concatenate([ref[i, k] for k in range(lanes)], axis=1)

    def first(g, side, h, t):
        lhs = jnp.concatenate([xall[g, pl.ds(h * T, T), :], aug[side, pl.ds(h * T, T), :]], axis=1)
        return jnp.dot(lhs, wide_load(rhs, t), preferred_element_type=F32)

    def weights(s, side, h, t, phase, masked, keep, row):
        top_t = top[t]
        acc = rs[phase, t]
        for p in range(T // PIECE):
            e = jnp.exp2(jnp.minimum(s(p).reshape(PIECE // 8, 8, chunk), top_t[None]) * scale).reshape(PIECE, chunk)
            rows_p = pl.ds(h * T + p * PIECE, PIECE)
            w = jnp.concatenate([qb[side, rows_p, :]] * lanes, axis=1) * e
            if masked:
                r = lax.broadcasted_iota(jnp.int32, (PIECE, chunk), 0) + (h * T + p * PIECE)
                w = jnp.where(r == lax.broadcasted_iota(jnp.int32, (PIECE, chunk), 1), 0.0, w)
            acc = acc + jnp.sum(w.reshape(PIECE // 8, 8, chunk), axis=0)
            if row is not None:
                ws = (w.reshape(PIECE // 8, 8, chunk) * sign[t][None]).reshape(PIECE, chunk)
                along = (ws[:, 0:128] + ws[:, 128:256]) + (ws[:, 256:384] + ws[:, 384:512])
                rcol[row, rows_p, :] = along if t == row + 1 else rcol[row, rows_p, :] + along
            w = w.astype(BF16)
            for j in range(lanes):
                wbuf[keep, j, rows_p, :] = w[:, j * 128:(j + 1) * 128]
        rs[phase, t] = acc

    def pull(side, t, keep, row):
        w = wide_load(wbuf, keep)
        ft[t] += jnp.dot(wide_load(xt, side), w, preferred_element_type=F32)
        if row is not None:
            back = lax.dot_general(wide_load(xs, t), w, (((1,), (1,)), ((), ())), preferred_element_type=F32)
            ft[row] += (back.reshape(feat // 8, 8, chunk) * sign[row][None]).reshape(feat, chunk)

    def row_sums():
        for c in range(own - 1):
            rs[0, c] += jnp.sum(rcol[c].T.reshape(16, 8, chunk), axis=0) * sign[c]

    def body(g, nxt, side, groups, previous, upcoming, hooks, arrive):
        steps = [(k, h) for k in range(len(groups)) for h in range(2)]
        ready = lambda p: sbuf[pl.ds(p * PIECE, PIECE), :]
        for n, (k, h) in enumerate(steps):
            t, phase, masked, row, keep = groups[k]
            if n == 1 and arrive is not None:
                arrive()
            if n + 1 < len(steps):
                following = first(g, side, steps[n + 1][1], groups[steps[n + 1][0]][0])
            if h == 0 and previous is not None:
                pull(*previous)
            if n == (0 if arrive is None else 1) and nxt is not None:
                prepare(nxt, 1 - side)
            if n in hooks:
                hooks[n]()
            weights(ready, side, h, t, phase, masked, keep, row)
            ready = lambda p, v=following: v[p * PIECE:(p + 1) * PIECE]
            if h == 1:
                previous = (side, t, keep, row)
        if nxt is not None:
            sbuf[...] = first(nxt, 1 - side, 0, upcoming)
        return previous

    rs[...] = jnp.zeros_like(rs)
    ft[...] = jnp.zeros_like(ft)
    local[0].wait()
    for c in range(own):
        local[1 + c].wait()
        q_c = q_row(c)
        sign[c] = jnp.broadcast_to(jnp.where(q_c < 0.0, -1.0, 1.0), (8, chunk))
        level = jnp.maximum(jnp.log2(jnp.abs(q_c)), -1000.0) * (1.0 / scale)
        top[c] = jnp.broadcast_to(level, (8, chunk))
        x_t = xall[c].T
        terms = [-1.0, -1.0, -1.0] + [v for v in split3(level - jnp.sum(jnp.square(x_t.astype(F32)), axis=0, keepdims=True))]
        block = jnp.zeros((8, chunk), F32)
        for k, v in enumerate(terms):
            block = jnp.where(row_id == k, v, block)
        block = jnp.concatenate([block, filler], axis=0).astype(BF16)
        double = x_t + x_t
        signed = x_t * jnp.where(q_c < 0.0, -1.0, 1.0).astype(BF16)
        for k in range(lanes):
            rhs[c, k, pl.ds(0, feat), :] = double[:, k * 128:(k + 1) * 128]
            xs[c, k] = signed[:, k * 128:(k + 1) * 128]
            rhs[c, k, pl.ds(feat, 128), :] = block[:, k * 128:(k + 1) * 128]
    pl.semaphore_wait(barrier, 3)
    for k in (1, 2, 0):
        q_copies[k].start()
    for copy in x_copies[:own // 2] + [p_copy]:
        copy.start()
    prepare(0, 0)
    sbuf[...] = first(0, 0, 0, 0)

    def total_of(phase):
        sums = (rs[phase, 0] * sign[0] + rs[phase, 1] * sign[1]) + (rs[phase, 2] * sign[2] + rs[phase, 3] * sign[3])
        return jnp.sum(jnp.sum(sums, axis=0, keepdims=True), axis=1, keepdims=True)
    e_copies = [remote(ebuf.at[me], ebuf.at[me], esend.at[k], erecv.at[k], peer) for k, peer in enumerate(peers)]

    def send_energy():
        for copy in e_copies:
            copy.start()

    def finish_part(t):
        sums = jnp.sum((rs[0, t] + rs[1, t]) + rs[2, t], axis=0, keepdims=True)
        mine = wide_load(xs, t).astype(F32)
        stage[t] = ((sums * mine - ft[t] * sign[t, pl.ds(0, 1), :]) * (1.0 / feat)).T

    def close_energy():
        ebuf[me] = jnp.broadcast_to(0.5 * total_of(0) + total_of(1), (8, 128))

    x_id, f_id, end = 2 * own, 3 * own, own - 1
    ids = list(range(2 * own)) + [x_id, x_id + 1, f_id, f_id + 1, x_id + 2, f_id + 2, x_id + 3, f_id + 3]
    x_waits = {x_id: (0,), x_id + 1: (1,), x_id + 2: (2,), x_id + 3: (3,)}
    f_waits = {f_id: (0, 1), f_id + 2: (2,), f_id + 3: (3,)}

    def arrivals(nxt):
        if nxt == own:
            q_copies[0].wait_recv()
            p_copy.wait_recv()
            for copy in x_copies[own // 2:]:
                copy.start()
        if nxt == x_id:
            q_copies[1].wait_recv()
            q_copies[2].wait_recv()
        for k in x_waits.get(nxt, ()):
            x_copies[k].wait_recv()
            f_copies[k].start()
        for k in f_waits.get(nxt, ()):
            f_copies[k].wait_recv()

    def phase_of(g, t):
        if g < x_id:
            return 0
        if g < x_id + end or (t == end and g < f_id + end):
            return 1
        return 2

    count, previous = 0, None
    for n, g in enumerate(ids):
        nxt = ids[n + 1] if n + 1 < len(ids) else None
        awaited = nxt == own or nxt in x_waits or nxt in f_waits
        first_t = lambda m, i: m if m < own else end if i == x_id + end else 0
        hooks = {own: {2: row_sums}, 2 * own + 6: {2: close_energy, 5: send_energy}}.get(n, {})
        if nxt is None:
            hooks = {2 * t + 3: functools.partial(finish_part, t) for t in range(own - 1)}
        groups = []
        for k in range(own - n if n < own else own):
            t = n + k if n < own else (first_t(n, g) + k) % own
            groups.append((t, phase_of(g, t), t == n and n < own, n if n < own and t > n else None, count % 2))
            count += 1
        previous = body(g, nxt, n % 2, groups, previous, first_t(n + 1, nxt), hooks,
                        functools.partial(arrivals, nxt) if awaited else None)
    pull(*previous)

    rs[0, end] = (rs[0, end] + rs[1, end]) + rs[2, end]
    rs[1, end] = sign[end]
    for copy in e_copies:
        copy.wait_recv()
    for copy in e_copies + q_copies + [p_copy] + x_copies + f_copies:
        copy.wait_send()


def finish(x_ref, ft, rs, ebuf, done, f_ref, e_ref, tail, value, sems):
    own, feat, chunk = ft.shape
    end = own - 1
    parts = [pltpu.make_async_copy(done.at[t], f_ref.at[t], sems.at[t]) for t in range(end)]
    for copy in parts:
        copy.start()
    energy = (ebuf[0] + ebuf[1]) + (ebuf[2] + ebuf[3])
    value[0] = jnp.max(energy[0:1, 0:1])
    copies = [pltpu.make_async_copy(value, e_ref, sems.at[own])]
    copies[0].start()
    sums = jnp.sum(rs[0, end], axis=0, keepdims=True)
    factor = rs[1, end, pl.ds(0, 1), :] * (1.0 / feat)
    tail[...] = ((sums * x_ref[end].T.astype(F32) - ft[end]) * factor).T
    copies.append(pltpu.make_async_copy(tail, f_ref.at[end], sems.at[end]))
    copies[-1].start()
    copies += parts
    for copy in copies:
        copy.wait()


def solution(mesh):
    def device_body(pos_loc, chg_loc):
        rows, feat = pos_loc.shape
        chunk = 2 * T
        own = rows // chunk
        total = 4 * own
        DMA = pltpu.SemaphoreType.DMA
        call = pl.pallas_call(
            functools.partial(kernel, rows, feat),
            out_shape=[jax.ShapeDtypeStruct((own, feat, chunk), F32), jax.ShapeDtypeStruct((3, own, 8, chunk), F32),
                       jax.ShapeDtypeStruct((4, 8, 128), F32), jax.ShapeDtypeStruct((own, chunk, feat), F32)],
            in_specs=[pl.BlockSpec(memory_space=pl.ANY)] * 2,
            out_specs=[pl.BlockSpec(memory_space=pltpu.VMEM)] * 4,
            scratch_shapes=[
                pltpu.VMEM((total, chunk, feat), BF16),
                pltpu.VMEM((4 * rows // 128, 128), F32),
                pltpu.VMEM((2, chunk, 128), BF16),
                pltpu.VMEM((2, chunk // 128, feat, 128), BF16),
                pltpu.VMEM((2, chunk, 128), F32),
                pltpu.VMEM((own, chunk // 128, 2 * 128, 128), BF16),
                pltpu.VMEM((own, 8, chunk), F32),
                pltpu.VMEM((own, 8, chunk), F32),
                pltpu.VMEM((own, chunk // 128, feat, 128), BF16),
                pltpu.VMEM((own - 1, chunk, 128), F32),
                pltpu.VMEM((T, chunk), F32),
                pltpu.VMEM((2, chunk // 128, chunk, 128), BF16),
                DMA((own + 1,)), DMA((own,)), DMA((own,)), DMA((own,)), DMA((own,)), DMA, DMA, DMA((3,)), DMA((3,)), DMA((3,)), DMA((3,)),
            ],
            compiler_params=pltpu.CompilerParams(collective_id=0, has_side_effects=True, vmem_limit_bytes=48 * 1024 * 1024),
        )
        x_blocks = pos_loc.reshape(own, chunk, feat)
        pulled, sums, parts, done = call(pltpu.with_memory_space_constraint(x_blocks, pltpu.HBM),
                                   pltpu.with_memory_space_constraint(chg_loc.reshape(rows // 128, 128), pltpu.HBM))
        force, energy = pl.pallas_call(
            finish,
            out_shape=[jax.ShapeDtypeStruct((own, chunk, feat), F32), jax.ShapeDtypeStruct((1,), F32)],
            in_specs=[pl.BlockSpec(memory_space=pltpu.VMEM)] * 5,
            out_specs=[pl.BlockSpec(memory_space=pltpu.HBM)] * 2,
            scratch_shapes=[pltpu.VMEM((chunk, feat), F32), pltpu.SMEM((1,), F32), DMA((own + 1,))],
            compiler_params=pltpu.CompilerParams(vmem_limit_bytes=8 * 1024 * 1024),
        )(x_blocks, pulled, sums, parts, done)
        return force.reshape(rows, feat), energy

    return jax.shard_map(device_body, mesh=mesh, in_specs=(P(("sys", "row"), None), P(("sys", "row"))), out_specs=(P(("sys", "row"), None), P("sys")), check_vma=False)
```

```python
import functools
import math

import jax
import jax.numpy as jnp
from jax import lax
from jax.experimental import pallas as pl
from jax.experimental.pallas import tpu as pltpu
from jax.sharding import PartitionSpec as P

MESH = pl.DeviceIdType.MESH
T = 256
F32 = jnp.float32
BF16 = jnp.bfloat16
PIECE = 64


def split3(v):
    hi = v.astype(BF16).astype(F32)
    rest = v - hi
    mid = rest.astype(BF16).astype(F32)
    return hi, mid, rest - mid


def kernel(rows, feat, x_ref, q_ref, ft, rs, ebuf, stage, xall, qall, aug, xt, qb, rhs, top, sign, xs, rcol, sbuf, wbuf,
           lsem, xsend, xrecv, fsend, frecv, psend, precv, qsend, qrecv, esend, erecv):
    me = lax.axis_index("row")
    upper = me // 2
    partner = me + 1 - 2 * lax.rem(me, 2)
    third = (1 - upper) * (3 - me) + upper * (me - 2)
    last = third + 1 - 2 * lax.rem(third, 2)
    peers = (partner, third, last)
    chunk = 2 * T
    own = rows // chunk
    total = 4 * own
    lanes = chunk // 128
    scale = math.log2(math.e) / (2.0 * feat)

    local = [pltpu.make_async_copy(q_ref, qall.at[pl.ds(0, own * lanes)], lsem.at[own])]
    local += [pltpu.make_async_copy(x_ref.at[c], xall.at[c], lsem.at[c]) for c in range(own)]
    for copy in local:
        copy.start()
    barrier = pltpu.get_barrier_semaphore()
    for peer in peers:
        pl.semaphore_signal(barrier, inc=1, device_id={"row": peer}, device_id_type=MESH)

    def remote(src, dst, ssem, rsem, peer):
        return pltpu.make_async_remote_copy(src_ref=src, dst_ref=dst, send_sem=ssem, recv_sem=rsem,
                                            device_id={"row": peer}, device_id_type=MESH)

    q_copies = [remote(q_ref, qall.at[pl.ds((k + 1) * own * lanes, own * lanes)], qsend.at[k], qrecv.at[k], peer)
                for k, peer in enumerate(peers)]
    p_copy = remote(xall.at[pl.ds(0, own)], xall.at[pl.ds(own, own)], psend, precv, partner)
    x_copies = [remote(xall.at[k], xall.at[2 * own + k], xsend.at[k], xrecv.at[k], third) for k in range(own)]
    f_copies = [remote(xall.at[2 * own + k], xall.at[3 * own + k], fsend.at[k], frecv.at[k], partner) for k in range(own)]

    row_id = lax.broadcasted_iota(jnp.int32, (8, chunk), 0)
    filler = jnp.zeros((120, chunk), F32)

    def norms(x_t):
        wide = x_t.astype(F32)
        return split3(jnp.sum(wide * wide, axis=0, keepdims=True))

    def q_row(g):
        return qall[pl.ds(g * lanes, lanes), :].reshape(1, chunk)

    def prepare(g, side):
        x_t = xall[g].T
        hi, mid, lo = norms(x_t)
        block = jnp.where(row_id == 0, hi, jnp.where(row_id == 1, mid, jnp.where(row_id == 2, lo, jnp.where(row_id < 6, 1.0, 0.0))))
        aug[side] = jnp.concatenate([block, filler], axis=0).astype(BF16).T
        qb[side] = jnp.broadcast_to(q_row(g), (128, chunk)).T
        for k in range(lanes):
            xt[side, k] = x_t[:, k * 128:(k + 1) * 128]

    def wide_load(ref, i):
        return jnp.concatenate([ref[i, k] for k in range(lanes)], axis=1)

    def first(g, side, h, t):
        lhs = jnp.concatenate([xall[g, pl.ds(h * T, T), :], aug[side, pl.ds(h * T, T), :]], axis=1)
        return jnp.dot(lhs, wide_load(rhs, t), preferred_element_type=F32)

    def weights(s, side, h, t, phase, masked, keep, row):
        top_t = top[t]
        acc = rs[phase, t]
        for p in range(T // PIECE):
            e = jnp.exp2(jnp.minimum(s(p).reshape(PIECE // 8, 8, chunk), top_t[None]) * scale).reshape(PIECE, chunk)
            rows_p = pl.ds(h * T + p * PIECE, PIECE)
            w = jnp.concatenate([qb[side, rows_p, :]] * lanes, axis=1) * e
            if masked:
                r = lax.broadcasted_iota(jnp.int32, (PIECE, chunk), 0) + (h * T + p * PIECE)
                w = jnp.where(r == lax.broadcasted_iota(jnp.int32, (PIECE, chunk), 1), 0.0, w)
            acc = acc + jnp.sum(w.reshape(PIECE // 8, 8, chunk), axis=0)
            if row is not None:
                ws = (w.reshape(PIECE // 8, 8, chunk) * sign[t][None]).reshape(PIECE, chunk)
                along = (ws[:, 0:128] + ws[:, 128:256]) + (ws[:, 256:384] + ws[:, 384:512])
                rcol[row, rows_p, :] = along if t == row + 1 else rcol[row, rows_p, :] + along
            w = w.astype(BF16)
            for j in range(lanes):
                wbuf[keep, j, rows_p, :] = w[:, j * 128:(j + 1) * 128]
        rs[phase, t] = acc

    def pull(side, t, keep, row):
        w = wide_load(wbuf, keep)
        ft[t] += jnp.dot(wide_load(xt, side), w, preferred_element_type=F32)
        if row is not None:
            back = lax.dot_general(wide_load(xs, t), w, (((1,), (1,)), ((), ())), preferred_element_type=F32)
            ft[row] += (back.reshape(feat // 8, 8, chunk) * sign[row][None]).reshape(feat, chunk)

    def row_sums():
        for c in range(own - 1):
            rs[0, c] += jnp.sum(rcol[c].T.reshape(16, 8, chunk), axis=0) * sign[c]

    def body(g, nxt, side, groups, previous, upcoming, hooks, arrive):
        steps = [(k, h) for k in range(len(groups)) for h in range(2)]
        ready = lambda p: sbuf[pl.ds(p * PIECE, PIECE), :]
        for n, (k, h) in enumerate(steps):
            t, phase, masked, row, keep = groups[k]
            if n == 1 and arrive is not None:
                arrive()
            if n + 1 < len(steps):
                following = first(g, side, steps[n + 1][1], groups[steps[n + 1][0]][0])
            if h == 0 and previous is not None:
                pull(*previous)
            if n == (0 if arrive is None else 1) and nxt is not None:
                prepare(nxt, 1 - side)
            if n in hooks:
                hooks[n]()
            weights(ready, side, h, t, phase, masked, keep, row)
            ready = lambda p, v=following: v[p * PIECE:(p + 1) * PIECE]
            if h == 1:
                previous = (side, t, keep, row)
        if nxt is not None:
            sbuf[...] = first(nxt, 1 - side, 0, upcoming)
        return previous

    rs[...] = jnp.zeros_like(rs)
    ft[...] = jnp.zeros_like(ft)
    local[0].wait()
    for c in range(own):
        local[1 + c].wait()
        q_c = q_row(c)
        sign[c] = jnp.broadcast_to(jnp.where(q_c < 0.0, -1.0, 1.0), (8, chunk))
        level = jnp.maximum(jnp.log2(jnp.abs(q_c)), -1000.0) * (1.0 / scale)
        top[c] = jnp.broadcast_to(level, (8, chunk))
        x_t = xall[c].T
        terms = [-1.0, -1.0, -1.0] + [v for v in split3(level - jnp.sum(jnp.square(x_t.astype(F32)), axis=0, keepdims=True))]
        block = jnp.zeros((8, chunk), F32)
        for k, v in enumerate(terms):
            block = jnp.where(row_id == k, v, block)
        block = jnp.concatenate([block, filler], axis=0).astype(BF16)
        double = x_t + x_t
        signed = x_t * jnp.where(q_c < 0.0, -1.0, 1.0).astype(BF16)
        for k in range(lanes):
            rhs[c, k, pl.ds(0, feat), :] = double[:, k * 128:(k + 1) * 128]
            xs[c, k] = signed[:, k * 128:(k + 1) * 128]
            rhs[c, k, pl.ds(feat, 128), :] = block[:, k * 128:(k + 1) * 128]
    pl.semaphore_wait(barrier, 3)
    for k in (1, 2, 0):
        q_copies[k].start()
    for copy in x_copies[:own // 2] + [p_copy]:
        copy.start()
    prepare(0, 0)
    sbuf[...] = first(0, 0, 0, 0)

    def total_of(phase):
        sums = (rs[phase, 0] * sign[0] + rs[phase, 1] * sign[1]) + (rs[phase, 2] * sign[2] + rs[phase, 3] * sign[3])
        return jnp.sum(jnp.sum(sums, axis=0, keepdims=True), axis=1, keepdims=True)
    e_copies = [remote(ebuf.at[me], ebuf.at[me], esend.at[k], erecv.at[k], peer) for k, peer in enumerate(peers)]

    def send_energy():
        for copy in e_copies:
            copy.start()

    def finish_part(t):
        sums = jnp.sum((rs[0, t] + rs[1, t]) + rs[2, t], axis=0, keepdims=True)
        mine = wide_load(xs, t).astype(F32)
        stage[t] = ((sums * mine - ft[t] * sign[t, pl.ds(0, 1), :]) * (1.0 / feat)).T

    def close_energy():
        ebuf[me] = jnp.broadcast_to(0.5 * total_of(0) + total_of(1), (8, 128))

    x_id, f_id, end = 2 * own, 3 * own, own - 1
    ids = list(range(2 * own)) + [x_id, x_id + 1, f_id, f_id + 1, x_id + 2, x_id + 3, f_id + 2, f_id + 3]
    x_waits = {x_id: (0,), x_id + 1: (1,), x_id + 2: (2,), x_id + 3: (3,)}
    f_waits = {f_id: (0, 1), f_id + 2: (2,), f_id + 3: (3,)}

    def arrivals(nxt):
        if nxt == own:
            q_copies[0].wait_recv()
            p_copy.wait_recv()
            for copy in x_copies[own // 2:]:
                copy.start()
        if nxt == x_id:
            q_copies[1].wait_recv()
            q_copies[2].wait_recv()
        for k in x_waits.get(nxt, ()):
            x_copies[k].wait_recv()
            f_copies[k].start()
        for k in f_waits.get(nxt, ()):
            f_copies[k].wait_recv()

    def phase_of(g, t):
        if g < x_id:
            return 0
        whole = g < x_id + end
        rest = t >= own // 2 if g == x_id + end else t == end and g < f_id + own // 2
        return 1 if whole or rest else 2

    count, previous = 0, None
    for n, g in enumerate(ids):
        nxt = ids[n + 1] if n + 1 < len(ids) else None
        awaited = nxt == own or nxt in x_waits or nxt in f_waits
        first_t = lambda m, i: m if m < own else own // 2 if i == x_id + end else 0
        hooks = {own: {2: row_sums}, 2 * own + 5: {4: close_energy, 6: send_energy}}.get(n, {})
        if nxt is None:
            hooks = {2 * t + 3: functools.partial(finish_part, t) for t in range(own - 1)}
        groups = []
        for k in range(own - n if n < own else own):
            t = n + k if n < own else (first_t(n, g) + k) % own
            groups.append((t, phase_of(g, t), t == n and n < own, n if n < own and t > n else None, count % 2))
            count += 1
        previous = body(g, nxt, n % 2, groups, previous, first_t(n + 1, nxt), hooks,
                        functools.partial(arrivals, nxt) if awaited else None)
    pull(*previous)

    rs[0, end] = (rs[0, end] + rs[1, end]) + rs[2, end]
    rs[1, end] = sign[end]
    for copy in e_copies:
        copy.wait_recv()
    for copy in e_copies + q_copies + [p_copy] + x_copies + f_copies:
        copy.wait_send()


def finish(x_ref, ft, rs, ebuf, done, f_ref, e_ref, tail, value, sems):
    own, feat, chunk = ft.shape
    end = own - 1
    parts = [pltpu.make_async_copy(done.at[t], f_ref.at[t], sems.at[t]) for t in range(end)]
    for copy in parts:
        copy.start()
    energy = (ebuf[0] + ebuf[1]) + (ebuf[2] + ebuf[3])
    value[0] = jnp.max(energy[0:1, 0:1])
    copies = [pltpu.make_async_copy(value, e_ref, sems.at[own])]
    copies[0].start()
    sums = jnp.sum(rs[0, end], axis=0, keepdims=True)
    factor = rs[1, end, pl.ds(0, 1), :] * (1.0 / feat)
    tail[...] = ((sums * x_ref[end].T.astype(F32) - ft[end]) * factor).T
    copies.append(pltpu.make_async_copy(tail, f_ref.at[end], sems.at[end]))
    copies[-1].start()
    copies += parts
    for copy in copies:
        copy.wait()


def solution(mesh):
    def device_body(pos_loc, chg_loc):
        rows, feat = pos_loc.shape
        chunk = 2 * T
        own = rows // chunk
        total = 4 * own
        DMA = pltpu.SemaphoreType.DMA
        call = pl.pallas_call(
            functools.partial(kernel, rows, feat),
            out_shape=[jax.ShapeDtypeStruct((own, feat, chunk), F32), jax.ShapeDtypeStruct((3, own, 8, chunk), F32),
                       jax.ShapeDtypeStruct((4, 8, 128), F32), jax.ShapeDtypeStruct((own, chunk, feat), F32)],
            in_specs=[pl.BlockSpec(memory_space=pl.ANY)] * 2,
            out_specs=[pl.BlockSpec(memory_space=pltpu.VMEM)] * 4,
            scratch_shapes=[
                pltpu.VMEM((total, chunk, feat), BF16),
                pltpu.VMEM((4 * rows // 128, 128), F32),
                pltpu.VMEM((2, chunk, 128), BF16),
                pltpu.VMEM((2, chunk // 128, feat, 128), BF16),
                pltpu.VMEM((2, chunk, 128), F32),
                pltpu.VMEM((own, chunk // 128, 2 * 128, 128), BF16),
                pltpu.VMEM((own, 8, chunk), F32),
                pltpu.VMEM((own, 8, chunk), F32),
                pltpu.VMEM((own, chunk // 128, feat, 128), BF16),
                pltpu.VMEM((own - 1, chunk, 128), F32),
                pltpu.VMEM((T, chunk), F32),
                pltpu.VMEM((2, chunk // 128, chunk, 128), BF16),
                DMA((own + 1,)), DMA((own,)), DMA((own,)), DMA((own,)), DMA((own,)), DMA, DMA, DMA((3,)), DMA((3,)), DMA((3,)), DMA((3,)),
            ],
            compiler_params=pltpu.CompilerParams(collective_id=0, has_side_effects=True, vmem_limit_bytes=48 * 1024 * 1024),
        )
        x_blocks = pos_loc.reshape(own, chunk, feat)
        pulled, sums, parts, done = call(pltpu.with_memory_space_constraint(x_blocks, pltpu.HBM),
                                   pltpu.with_memory_space_constraint(chg_loc.reshape(rows // 128, 128), pltpu.HBM))
        force, energy = pl.pallas_call(
            finish,
            out_shape=[jax.ShapeDtypeStruct((own, chunk, feat), F32), jax.ShapeDtypeStruct((1,), F32)],
            in_specs=[pl.BlockSpec(memory_space=pltpu.VMEM)] * 5,
            out_specs=[pl.BlockSpec(memory_space=pltpu.HBM)] * 2,
            scratch_shapes=[pltpu.VMEM((chunk, feat), F32), pltpu.SMEM((1,), F32), DMA((own + 1,))],
            compiler_params=pltpu.CompilerParams(vmem_limit_bytes=8 * 1024 * 1024),
        )(x_blocks, pulled, sums, parts, done)
        return force.reshape(rows, feat), energy

    return jax.shard_map(device_body, mesh=mesh, in_specs=(P(("sys", "row"), None), P(("sys", "row"))), out_specs=(P(("sys", "row"), None), P("sys")), check_vma=False)
```
